256 devices in a mesh: grid: 32 (over y, x, core), pair: 8 (over z).
Axes of the slice: x: 4, y: 4, z: 8, core: 2. Of those that a mesh axis runs over, the one named last changes fastest.
Arguments:
- orbitals: bfloat16 [64, 128, 4096], P('grid', None, 'pair'), may hold values from -6 to 6
- box_list: int32 [32, 8, 4], replicated, may hold values from 0 to 127, all different within a row
- pair_slots: int32 [32, 8, 4, 2], P('grid', 'pair'), may hold values from 0 to 3, as said below
- offsets: int32 [32, 8, 4, 3], P('grid', 'pair'), may hold values from -8 to 8
- pair_count: int32 [32, 8], P('grid', 'pair'), may hold values from 2 to 4, as said below
Outputs:
- exchange_field: float32 [64, 128, 4096], P('grid', None, 'pair')
The draws below stay inside these ranges and needn't reach their ends.
Inputs may be any that keep to these rules, and one draw needn't show every extreme that they name: `box_list`: the 4 orbitals of one worker's list are all different. `pair_slots`: only the first pair_count entries of a worker's lists are used; the first 2 pairs of every worker name each slot of its list exactly once. `pair_count`: each group of 8 workers that share a grid index holds 24 pairs, and one of them holds 4.
All inputs are finite; a program needn't handle non-finite values.
Results may differ from the reference program's by a relative error of at most 0.0019.
Values may be sent and summed in bfloat16 or wider, within the bound.
A program may use at most 64 MiB of HBM per device.

```python
import math
import jax
import jax.numpy as jnp
from jax import lax

BOX = 64
CAPB = 4
NORB = 128
PAIR_MEAN = 3
MOSTP = 4
SHIFT = 8
N_GRID = 32
N_PAIR = 8


def draw_pair_slots(key, part):
    worker_total = N_GRID * N_PAIR
    worker_keys = jax.random.split(jax.random.fold_in(key, 7), worker_total)

    def one_order(worker_key):
        return jax.random.permutation(worker_key, CAPB).astype(jnp.int32)
    orders = jax.vmap(one_order)(worker_keys)
    leading = orders.reshape(worker_total, CAPB // 2, 2)
    remaining = jax.random.randint(jax.random.fold_in(key, 8), (worker_total, MOSTP - CAPB // 2, 2), 0, CAPB, dtype=jnp.int32)
    joined = jnp.concatenate([leading, remaining], axis=1)
    return joined.reshape(N_GRID, N_PAIR, MOSTP, 2).astype(jnp.int32)


def draw_pair_count(key, part):
    floor_count = CAPB // 2
    highest = MOSTP - floor_count
    spare = N_PAIR * (PAIR_MEAN - floor_count) - highest
    worker_ids = jnp.arange(N_PAIR, dtype=jnp.int32)

    def one_row(row_id):
        row_key = jax.random.fold_in(jax.random.fold_in(key, 11), row_id)
        chosen = jax.random.randint(jax.random.fold_in(row_key, 1), (), 0, N_PAIR, dtype=jnp.int32)
        offset_pick = jax.random.randint(jax.random.fold_in(row_key, 2), (), 0, N_PAIR - 1, dtype=jnp.int32)
        spare_units = jnp.arange(spare, dtype=jnp.int32)
        ranked = (offset_pick + spare_units) % (N_PAIR - 1)
        target = ranked + (ranked >= chosen).astype(jnp.int32)
        extra_pairs = jnp.sum((target[:, None] == worker_ids[None, :]).astype(jnp.int32), axis=0)
        extra_pairs = jnp.where(worker_ids == chosen, highest, extra_pairs)
        return (floor_count + extra_pairs).astype(jnp.int32)
    row_ids = jnp.arange(N_GRID, dtype=jnp.int32)
    return jax.vmap(one_row)(row_ids).astype(jnp.int32)


def set_ends(values, key, least, largest):
    shape = values.shape
    place = [jax.random.randint(jax.random.fold_in(key, axis), (), 0, shape[axis]) for axis in range(len(shape))]
    values = values.at[tuple(place)].set(least)
    longest = shape.index(max(shape))
    place[longest] = (place[longest] + 1) % shape[longest]
    return values.at[tuple(place)].set(largest)


def block_levels(rng, shape, cuts, low, high):
    level = 1.0
    for position, parts in cuts:
        steps = jax.random.uniform(jax.random.fold_in(jax.random.fold_in(rng, 6), position), (parts,), jnp.float32, low / len(cuts), high / len(cuts))
        level = level * jnp.repeat(jnp.exp(steps), shape[position] // parts).reshape((-1,) + (1,) * (len(shape) - 1 - position))
    return level


def different_ones(rng, rows, amount, top, lift):
    order = jax.random.permutation(jax.random.fold_in(rng, 1), amount)
    boost = order
    for power in range(3):
        boost = boost * boost // amount
    boost = boost * lift // amount
    tickets = jax.random.randint(jax.random.fold_in(rng, 2), (rows, amount), 0, 4096) + boost
    sure = jax.random.permutation(jax.random.fold_in(rng, 3), rows)[jnp.arange(amount) % rows]
    tickets = jnp.where(jnp.arange(rows)[:, None] == sure[None, :], 1 << 14, tickets)
    score = tickets * amount + jnp.arange(amount)
    return lax.top_k(score.astype(jnp.int32), top)[1].astype(jnp.int32)


def gaussian(rng, dims, deviation, most, pieces=(), held_as=jnp.bfloat16):
    entries = deviation * jax.random.normal(rng, dims, jnp.float32)
    if pieces:
        entries = entries * block_levels(rng, dims, pieces, -0.22, 0.18)
    return jnp.clip(entries, -most, most).astype(held_as)


def setup_inputs(seed: int = 0) -> dict:
    splits = jax.random.split(jax.random.key(seed), 6)
    return {
        "orbitals": gaussian(splits[0], (BOX, NORB, BOX * BOX), 1.0, 6.0, ((0, 32), (2, 8))),
        "box_list": different_ones(splits[1], N_GRID * N_PAIR, NORB, CAPB, 256).reshape((N_GRID, N_PAIR, CAPB)),
        "pair_slots": draw_pair_slots(jax.random.fold_in(splits[5], 71), 0),
        "offsets": set_ends(jax.random.randint(splits[3], (N_GRID, N_PAIR, MOSTP, 3), -SHIFT, SHIFT + 1), jax.random.fold_in(splits[3], 1), -SHIFT, SHIFT).astype(jnp.int32),
        "pair_count": draw_pair_count(jax.random.fold_in(splits[5], 71), 0),
    }


screening = 0.02


def cas_table(extent):
    places = jnp.arange(extent, dtype=jnp.int32)
    product = (places[:, None] * places[None, :]) % extent
    phases = product.astype(jnp.float32) * (2.0 * math.pi / extent)
    return jnp.cos(phases) + jnp.sin(phases)


def green_table(extent):
    phases = jnp.arange(extent, dtype=jnp.int32).astype(jnp.float32) * (2.0 * math.pi / extent)
    eigen = 2.0 - 2.0 * jnp.cos(phases)
    denominator = screening + eigen[:, None, None] + eigen[None, :, None] + eigen[None, None, :]
    return 1.0 / (denominator * float(extent ** 3))


def poisson(density, table, green):
    high = lax.Precision.HIGHEST
    spectrum = jnp.einsum("ax,xyz->ayz", table, density, precision=high)
    spectrum = jnp.einsum("by,ayz->abz", table, spectrum, precision=high)
    spectrum = jnp.einsum("cz,abz->abc", table, spectrum, precision=high)
    spectrum = spectrum * green
    spectrum = jnp.einsum("ax,xyz->ayz", table, spectrum, precision=high)
    spectrum = jnp.einsum("by,ayz->abz", table, spectrum, precision=high)
    return jnp.einsum("cz,abz->abc", table, spectrum, precision=high)


def shift_box(field, step_x, step_y, step_z):
    extent = field.shape[0]
    padded = jnp.pad(field, SHIFT)
    starts = (SHIFT + step_x, SHIFT + step_y, SHIFT + step_z)
    return lax.dynamic_slice(padded, starts, (extent, extent, extent))


def worker_fields(box_data, slot_list, offset_list, pair_total):
    extent = box_data.shape[0]
    capacity = box_data.shape[1]
    table = cas_table(extent)
    green = green_table(extent)

    def fetch(slot):
        picked = lax.dynamic_index_in_dim(box_data, slot, 1, False)
        return picked.astype(jnp.float32).reshape(extent, extent, extent)

    def add_slot(collected, slot, value):
        current = lax.dynamic_index_in_dim(collected, slot, 1, True)
        updated = current + value.reshape(extent, 1, extent * extent)
        return lax.dynamic_update_index_in_dim(collected, updated, slot, 1)

    def one_pair(turn, collected):
        first_slot = slot_list[turn, 0]
        second_slot = slot_list[turn, 1]
        offset = offset_list[turn]
        first_box = fetch(first_slot)
        second_box = fetch(second_slot)
        shifted = shift_box(second_box, offset[0], offset[1], offset[2])
        potential = poisson(first_box * shifted, table, green)
        collected = add_slot(collected, first_slot, -(potential * shifted))
        returned = shift_box(-(potential * first_box), -offset[0], -offset[1], -offset[2])
        return add_slot(collected, second_slot, returned)

    start = jnp.zeros((extent, capacity, extent * extent), jnp.float32)
    collected = lax.fori_loop(jnp.int32(0), pair_total.astype(jnp.int32), one_pair, start)
    return collected.astype(jnp.bfloat16)


def reference(orbitals, box_list, pair_slots, offsets, pair_count):
    extent = orbitals.shape[0]
    capacity = box_list.shape[2]
    workers = box_list.shape[0] * box_list.shape[1]
    lists = box_list.reshape(workers, capacity)
    slot_lists = pair_slots.reshape(workers, pair_slots.shape[2], 2)
    offset_lists = offsets.reshape(workers, offsets.shape[2], 3)
    totals = pair_count.reshape(workers)

    def visit(summed, worker_items):
        orbital_ids, slot_list, offset_list, pair_total = worker_items
        box_data = jnp.take(orbitals, orbital_ids, axis=1)
        fields = worker_fields(box_data, slot_list, offset_list, pair_total).astype(jnp.float32)
        return summed.at[:, orbital_ids, :].add(fields), None

    start = jnp.zeros((extent, orbitals.shape[1], extent * extent), jnp.float32)
    summed, _ = lax.scan(visit, start, (lists, slot_lists, offset_lists, totals))
    return summed
```

```python
import math
import numpy as np
import jax
import jax.numpy as jnp
from jax import lax
from jax.experimental import pallas as pl
from jax.experimental.pallas import tpu as pltpu
from jax.sharding import PartitionSpec as P

screening = 0.02
N = 64
CH = 16
W = 256
PITCH = 72
f32, bf16 = jnp.float32, jnp.bfloat16


def tables():
    m = np.arange(N)
    ph = 2.0 * math.pi * ((m[:, None] * m[None, :]) % N) / N
    cas = np.cos(ph) + np.sin(ph)
    perm = np.concatenate([np.arange(0, N, 2), np.arange(1, N, 2)])

    def parts(a):
        a = np.asarray(a, np.float32)
        hi = a.astype(bf16)
        lo = (a - hi.astype(np.float32)).astype(bf16)
        return hi, lo

    def left(a):
        hi, lo = parts(a)
        return np.concatenate([hi, hi, lo], axis=1)

    cx = left(cas)
    cf = left(cas[:, perm])
    ci = left(cas[perm, :])
    hi, lo = parts(np.kron(np.eye(4), cas))
    bd = np.concatenate([hi, hi, lo], axis=0)
    e = 2.0 - 2.0 * np.cos(2.0 * math.pi * m / N)
    green = 1.0 / ((screening + e[:, None, None] + e[None, :, None] + e[None, None, :]) * float(N**3))
    g = green.reshape(CH, 4, N, N).transpose(0, 2, 1, 3).reshape(CH, N, W).astype(np.float32)
    return cx, cf, ci, bd, g


def split(v):
    hi = v.astype(bf16)
    lo = (v - hi.astype(f32)).astype(bf16)
    return hi, lo


def mm(a, b):
    return jnp.dot(a, b, preferred_element_type=f32)


def left_mul(table, v):
    hi, lo = split(v)
    return mm(table, jnp.concatenate([hi, lo, hi], axis=0))


def right_mul(v, bd):
    hi, lo = split(v)
    return mm(jnp.concatenate([hi, lo, hi], axis=1), bd)


def pair_kernel(slots, offs, count, box, cx, cf, ci, bd, green, out, pad, sh, U, wh, wl, col):
    GR = 4
    low = lax.broadcasted_iota(jnp.int32, (32, 128), 1) < 64
    zpad = jnp.zeros((4, N, W), bf16)
    for r in (pad, wh, wl):
        r[0:4] = zpad
        r[20:24] = zpad
    col[...] = jnp.zeros(col.shape, f32)

    def pair(k, carry):
        a = slots[k, 0]
        b = slots[k, 1]
        dx, dy, dz = offs[k, 0], offs[k, 1], offs[k, 2]
        t = dy * 64 + dz
        q = (t + 1024) // 256 - 4
        r = t - 256 * q
        rows = lax.broadcasted_iota(jnp.int32, (W, W), 0)
        cols = lax.broadcasted_iota(jnp.int32, (W, W), 1)
        zc = cols % 64 + dz
        okc = (zc >= 0) & (zc < 64)
        one, zero = jnp.float32(1), jnp.float32(0)

        def mask(c):
            return jnp.where(c, one, zero).astype(bf16)

        fwd = jnp.concatenate([mask(okc & (rows == cols + r)), mask(okc & (rows == cols + r - 256))], axis=0)
        zr = rows % 64 + dz
        okr = (zr >= 0) & (zr < 64)
        b0 = mask(okr & (cols == rows + r))
        b1 = mask(okr & (cols == rows + r - 256))
        bwd = jnp.concatenate([b0, b0, b1, b1], axis=0)
        xr = lax.broadcasted_iota(jnp.int32, (N, N), 0)
        xc = lax.broadcasted_iota(jnp.int32, (N, N), 1)
        sx = mask(xc == xr + dx)
        sxt = mask(xr == xc + dx)

        pad[4:20] = box[b]

        def forward(g, c):
            lo_ = g * GR
            src0 = pad[pl.ds(lo_ + 4 + q, GR)].reshape(GR * N, W)
            src1 = pad[pl.ds(lo_ + 5 + q, GR)].reshape(GR * N, W)
            yz = mm(jnp.concatenate([src0, src1], axis=1), fwd).astype(bf16).reshape(GR, N, W)
            outs = []
            for i in range(GR):
                s = mm(sx, yz[i])
                sh[lo_ + i] = s.astype(bf16)
                dens = box[a, lo_ + i].astype(f32) * s
                outs.append(left_mul(cx[...], dens))
            spec = right_mul(jnp.concatenate(outs, axis=0), bd[...])
            for i in range(GR):
                for h in range(2):
                    U[pl.ds(pl.multiple_of((2 * (lo_ + i) + h) * PITCH, 8), N), :] = spec[i * N:(i + 1) * N, h * 128:(h + 1) * 128]
            return c

        lax.fori_loop(0, CH // GR, forward, 0)

        def middle(g, c):
            tops, bots = [], []
            for h in range(2):
                l1 = U[pl.ds(g * 4 + 2 * h, 32, stride=PITCH), :]
                l2 = U[pl.ds(g * 4 + 2 * h + 1, 32, stride=PITCH), :]
                tops.append(jnp.where(low, l1, pltpu.roll(l2, 64, 1)))
                bots.append(jnp.where(low, pltpu.roll(l1, 64, 1), l2))
            v = jnp.concatenate([jnp.concatenate(tops, axis=1), jnp.concatenate(bots, axis=1)], axis=0)
            s = left_mul(cf[...], v) * green[g]
            p = left_mul(ci[...], s)
            for h in range(2):
                x0 = p[:32, h * 128:(h + 1) * 128]
                x1 = p[32:, h * 128:(h + 1) * 128]
                U[pl.ds(g * 4 + 2 * h, 32, stride=PITCH), :] = jnp.where(low, x0, pltpu.roll(x1, 64, 1))
                U[pl.ds(g * 4 + 2 * h + 1, 32, stride=PITCH), :] = jnp.where(low, pltpu.roll(x0, 64, 1), x1)
            return c

        lax.fori_loop(0, CH, middle, 0)

        def inverse(g, c):
            lo_ = g * GR
            outs = []
            for i in range(GR):
                v = jnp.concatenate(
                    [U[pl.ds(pl.multiple_of((2 * (lo_ + i) + h) * PITCH, 8), N), :] for h in range(2)], axis=1)
                outs.append(left_mul(cx[...], v))
            pot = right_mul(jnp.concatenate(outs, axis=0), bd[...]).reshape(GR, N, W)
            for i in range(GR):
                j = lo_ + i
                col[a, j] = col[a, j] - pot[i] * sh[j].astype(f32)
                hi, lo = split(-(pot[i] * box[a, j].astype(f32)))
                wh[j + 4] = mm(sxt, hi).astype(bf16)
                wl[j + 4] = mm(sxt, lo).astype(bf16)
            return c

        lax.fori_loop(0, CH // GR, inverse, 0)

        def back(g, c):
            lo_ = g * GR
            i0 = lo_ + 4 - q
            parts_ = [r_[pl.ds(i, GR)].reshape(GR * N, W) for i in (i0, i0 - 1) for r_ in (wh, wl)]
            u = mm(jnp.concatenate(parts_, axis=1), bwd)
            col[b, pl.ds(lo_, GR)] = col[b, pl.ds(lo_, GR)] + u.reshape(GR, N, W)
            return c

        lax.fori_loop(0, CH // GR, back, 0)
        return carry

    lax.fori_loop(0, count[0], pair, 0)
    out[...] = col[...].astype(bf16)


def worker_fields(box, slots, offs, count):
    cx, cf, ci, bd, g = (jnp.asarray(t) for t in tables())
    smem = pl.BlockSpec(memory_space=pltpu.SMEM)
    vmem = pl.BlockSpec(memory_space=pltpu.VMEM)
    return pl.pallas_call(
        pair_kernel,
        out_shape=jax.ShapeDtypeStruct((4, CH, N, W), bf16),
        in_specs=[smem] * 3 + [vmem] * 6,
        out_specs=vmem,
        scratch_shapes=[
            pltpu.VMEM((24, N, W), bf16),
            pltpu.VMEM((CH, N, W), bf16),
            pltpu.VMEM((32 * PITCH, 128), f32),
            pltpu.VMEM((24, N, W), bf16),
            pltpu.VMEM((24, N, W), bf16),
            pltpu.VMEM((4, CH, N, W), f32),
        ],
        compiler_params=pltpu.CompilerParams(vmem_limit_bytes=40 << 20),
        name="pairs",
    )(slots, offs, count, box, cx, cf, ci, bd, g)


def shards(orbitals, box_list, pair_slots, offsets, pair_count):
    planes, orbital_total, row_cells = orbitals.shape
    lists = box_list.reshape(-1)
    hot = (lists[:, None] == jnp.arange(orbital_total, dtype=jnp.int32)[None, :]).astype(bf16)
    local = orbitals.reshape(planes, orbital_total, 2, W)
    picked = jnp.einsum("ro,xojc->rjxc", hot, local, preferred_element_type=f32).astype(bf16)
    picked = picked.reshape(256, 4, 2, planes, W)
    arrived = lax.all_to_all(picked, ("grid", "pair"), split_axis=0, concat_axis=0, tiled=True)
    box = arrived.reshape(32, 8, 4, 2, planes, W).transpose(2, 1, 3, 0, 4, 5).reshape(4, CH, N, W)
    fields = worker_fields(box, pair_slots[0, 0], offsets[0, 0], pair_count[0])
    back = fields.reshape(4, 8, 2, 32, planes, W).transpose(3, 1, 0, 2, 4, 5).reshape(256, 4, 2, planes, W)
    landed = lax.all_to_all(back, ("grid", "pair"), split_axis=0, concat_axis=0, tiled=True)
    landed = landed.reshape(1024, 2, planes, W)
    summed = jnp.einsum("ro,rjxc->xojc", hot, landed, preferred_element_type=f32)
    return summed.reshape(planes, orbital_total, row_cells)


def solution(mesh):
    placed = (
        P("grid", None, "pair"),
        P(),
        P("grid", "pair", None, None),
        P("grid", "pair", None, None),
        P("grid", "pair"),
    )
    return jax.shard_map(
        shards, mesh=mesh, in_specs=placed, out_specs=P("grid", None, "pair"), check_vma=False
    )
```

```python
import math
import numpy as np
import jax
import jax.numpy as jnp
from jax import lax
from jax.experimental import pallas as pl
from jax.experimental.pallas import tpu as pltpu
from jax.sharding import PartitionSpec as P

screening = 0.02
N = 64
CH = 16
W = 256
PITCH = 72
f32, bf16 = jnp.float32, jnp.bfloat16


def tables():
    m = np.arange(N)
    ph = 2.0 * math.pi * ((m[:, None] * m[None, :]) % N) / N
    cas = np.cos(ph) + np.sin(ph)
    perm = np.concatenate([np.arange(0, N, 2), np.arange(1, N, 2)])

    def parts(a):
        a = np.asarray(a, np.float32)
        hi = a.astype(bf16)
        lo = (a - hi.astype(np.float32)).astype(bf16)
        return hi, lo

    def left(a):
        hi, lo = parts(a)
        return np.concatenate([hi, hi, lo], axis=1)

    cx = left(cas[:, perm])
    ux = left(cas[perm, :])
    cf = left(cas[:, perm])
    ci = left(cas[perm, :])
    hi, lo = parts(np.kron(np.eye(4), cas))
    bd = np.concatenate([hi, hi, lo], axis=0)
    e = 2.0 - 2.0 * np.cos(2.0 * math.pi * m / N)
    green = 1.0 / ((screening + e[:, None, None] + e[None, :, None] + e[None, None, :]) * float(N**3))
    g = green.reshape(CH, 4, N, N).transpose(0, 2, 1, 3).reshape(CH, N, W).astype(np.float32)
    return cx, ux, bd, g


def split(v):
    hi = v.astype(bf16)
    lo = (v - hi.astype(f32)).astype(bf16)
    return hi, lo


def mm(a, b):
    return jnp.dot(a, b, preferred_element_type=f32)


def left_mul(table, v):
    hi, lo = split(v)
    return mm(table, jnp.concatenate([hi, lo, hi], axis=0))


def right_mul(v, bd):
    hi, lo = split(v)
    return mm(jnp.concatenate([hi, lo, hi], axis=1), bd)


def pair_kernel(slots, offs, count, land, cx, ux, bd, green, out, box, pad, sh, U, F, wh, wl, col):
    GR = 4
    low = lax.broadcasted_iota(jnp.int32, (32, 128), 1) < 64
    zpad = jnp.zeros((4, N, W), bf16)
    for r in (pad, wh, wl):
        r[0:4] = zpad
        r[20:24] = zpad
    col[...] = jnp.zeros(col.shape, f32)
    place = lax.axis_index("pair")

    def arrange(s, c):
        def widen(g, c2):
            for k in range(8):
                F[pl.ds(pl.multiple_of(g * PITCH, 8) + 8 * k, 8), :] = land[k, g, s].astype(f32)
            return c2

        lax.fori_loop(0, 32, widen, 0)
        for k in range(8):
            j = (place + k) % 8 * 2
            for jj in range(2):
                for half in range(2):
                    two = [F[pl.ds(8 * k + 4 * jj + 2 * half + xx, 32, stride=PITCH), :] for xx in range(2)]
                    box[s, j + jj, :, half * 128:(half + 1) * 128] = jnp.concatenate(two, axis=0).astype(bf16)
        return c

    lax.fori_loop(0, 4, arrange, 0)

    def pair(k, carry):
        a = slots[k, 0]
        b = slots[k, 1]
        dx, dy, dz = offs[k, 0], offs[k, 1], offs[k, 2]
        t = dy * 64 + dz
        q = (t + 1024) // 256 - 4
        r = t - 256 * q
        rows = lax.broadcasted_iota(jnp.int32, (W, W), 0)
        cols = lax.broadcasted_iota(jnp.int32, (W, W), 1)
        zc = cols % 64 + dz
        okc = (zc >= 0) & (zc < 64)
        one, zero = jnp.float32(1), jnp.float32(0)

        def mask(c):
            return jnp.where(c, one, zero).astype(bf16)

        fwd = jnp.concatenate([mask(okc & (rows == cols + r)), mask(okc & (rows == cols + r - 256))], axis=0)
        zr = rows % 64 + dz
        okr = (zr >= 0) & (zr < 64)
        b0 = mask(okr & (cols == rows + r))
        b1 = mask(okr & (cols == rows + r - 256))
        bwd = jnp.concatenate([b0, b0, b1, b1], axis=0)
        xr = lax.broadcasted_iota(jnp.int32, (N, N), 0)
        xc = lax.broadcasted_iota(jnp.int32, (N, N), 1)
        xr = xr % 32 * 2 + xr // 32
        xc = xc % 32 * 2 + xc // 32
        sx = mask(xc == xr + dx)
        sxt = mask(xr == xc + dx)

        pad[4:20] = box[b]

        def forward(g, c):
            lo_ = g * GR
            src0 = pad[pl.ds(lo_ + 4 + q, GR)].reshape(GR * N, W)
            src1 = pad[pl.ds(lo_ + 5 + q, GR)].reshape(GR * N, W)
            yz = mm(jnp.concatenate([src0, src1], axis=1), fwd).astype(bf16).reshape(GR, N, W)
            outs = []
            for i in range(GR):
                s = mm(sx, yz[i])
                sh[lo_ + i] = s.astype(bf16)
                dens = box[a, lo_ + i].astype(f32) * s
                outs.append(left_mul(cx[...], dens))
            spec = right_mul(jnp.concatenate(outs, axis=0), bd[...])
            for i in range(GR):
                for h in range(2):
                    U[pl.ds(pl.multiple_of((2 * (lo_ + i) + h) * PITCH, 8), N), :] = spec[i * N:(i + 1) * N, h * 128:(h + 1) * 128]
            return c

        lax.fori_loop(0, CH // GR, forward, 0)

        def middle(g, c):
            tops, bots = [], []
            for h in range(2):
                l1 = U[pl.ds(g * 4 + 2 * h, 32, stride=PITCH), :]
                l2 = U[pl.ds(g * 4 + 2 * h + 1, 32, stride=PITCH), :]
                tops.append(jnp.where(low, l1, pltpu.roll(l2, 64, 1)))
                bots.append(jnp.where(low, pltpu.roll(l1, 64, 1), l2))
            v = jnp.concatenate([jnp.concatenate(tops, axis=1), jnp.concatenate(bots, axis=1)], axis=0)
            s = left_mul(cx[...], v) * green[g]
            p = left_mul(ux[...], s)
            for h in range(2):
                x0 = p[:32, h * 128:(h + 1) * 128]
                x1 = p[32:, h * 128:(h + 1) * 128]
                U[pl.ds(g * 4 + 2 * h, 32, stride=PITCH), :] = jnp.where(low, x0, pltpu.roll(x1, 64, 1))
                U[pl.ds(g * 4 + 2 * h + 1, 32, stride=PITCH), :] = jnp.where(low, pltpu.roll(x0, 64, 1), x1)
            return c

        lax.fori_loop(0, CH, middle, 0)

        def inverse(g, c):
            lo_ = g * GR
            outs = []
            for i in range(GR):
                v = jnp.concatenate(
                    [U[pl.ds(pl.multiple_of((2 * (lo_ + i) + h) * PITCH, 8), N), :] for h in range(2)], axis=1)
                outs.append(left_mul(ux[...], v))
            pot = right_mul(jnp.concatenate(outs, axis=0), bd[...]).reshape(GR, N, W)
            for i in range(GR):
                j = lo_ + i
                col[a, j] = col[a, j] - pot[i] * sh[j].astype(f32)
                hi, lo = split(-(pot[i] * box[a, j].astype(f32)))
                wh[j + 4] = mm(sxt, hi).astype(bf16)
                wl[j + 4] = mm(sxt, lo).astype(bf16)
            return c

        lax.fori_loop(0, CH // GR, inverse, 0)

        def back(g, c):
            lo_ = g * GR
            i0 = lo_ + 4 - q
            parts_ = [r_[pl.ds(i, GR)].reshape(GR * N, W) for i in (i0, i0 - 1) for r_ in (wh, wl)]
            u = mm(jnp.concatenate(parts_, axis=1), bwd)
            col[b, pl.ds(lo_, GR)] = col[b, pl.ds(lo_, GR)] + u.reshape(GR, N, W)
            return c

        lax.fori_loop(0, CH // GR, back, 0)
        return carry

    lax.fori_loop(0, count[0], pair, 0)

    def deliver(s, c):
        for k in range(8):
            for jj in range(2):
                for half in range(2):
                    for xx in range(2):
                        F[pl.ds(8 * k + 4 * jj + 2 * half + xx, 32, stride=PITCH), :] = (
                            col[s, 2 * k + jj, xx * 32:(xx + 1) * 32, half * 128:(half + 1) * 128])

        def narrow(g, c2):
            for k in range(8):
                out[g, k, s] = F[pl.ds(pl.multiple_of(g * PITCH, 8) + 8 * k, 8), :].astype(bf16)
            return c2

        lax.fori_loop(0, 32, narrow, 0)
        return c

    lax.fori_loop(0, 4, deliver, 0)


def worker_fields(land, slots, offs, count):
    cx, ux, bd, g = (jnp.asarray(t) for t in tables())
    smem = pl.BlockSpec(memory_space=pltpu.SMEM)
    vmem = pl.BlockSpec(memory_space=pltpu.VMEM)
    return pl.pallas_call(
        pair_kernel,
        out_shape=jax.ShapeDtypeStruct((32, 8, 4, 8, 128), bf16),
        in_specs=[smem] * 3 + [vmem] * 5,
        out_specs=vmem,
        scratch_shapes=[
            pltpu.VMEM((4, CH, N, W), bf16),
            pltpu.VMEM((24, N, W), bf16),
            pltpu.VMEM((CH, N, W), bf16),
            pltpu.VMEM((32 * PITCH, 128), f32),
            pltpu.VMEM((32 * PITCH, 128), f32),
            pltpu.VMEM((24, N, W), bf16),
            pltpu.VMEM((24, N, W), bf16),
            pltpu.VMEM((4, CH, N, W), f32),
        ],
        compiler_params=pltpu.CompilerParams(vmem_limit_bytes=40 << 20),
        name="pairs",
    )(slots, offs, count, land, cx, ux, bd, g)


MESH = pl.DeviceIdType.MESH
SUBS = 4


def gather_kernel(gy, gx, orb, lists, land, *rest):
    blocks = rest[:7]
    send, zsend, zrecv, ssem, rsem = rest[7:]
    G = gy * gx * 2
    me = lax.axis_index("grid")
    p = lax.axis_index("pair")
    my_y, my_x, my_c = me // (2 * gx), (me // 2) % gx, me % 2
    right, left = (p + 1) % 8, (p + 7) % 8
    held = (orb,) + tuple(blocks)
    rows = orb.shape[0] // SUBS

    def peer(i):
        y = (my_y + i // (2 * gx)) % gy
        x = (my_x + (i // 2) % gx) % gx
        c = (my_c + i) % 2
        return (y * gx + x) * 2 + c

    barrier = pltpu.get_barrier_semaphore()
    pl.semaphore_signal(barrier, inc=1, device_id=(me, right), device_id_type=MESH)
    pl.semaphore_signal(barrier, inc=1, device_id=(me, left), device_id_type=MESH)

    def greet(i, c):
        pl.semaphore_signal(barrier, inc=1, device_id=(peer(i), p), device_id_type=MESH)
        return c

    lax.fori_loop(1, G, greet, 0)
    pl.semaphore_wait(barrier, G + 1)

    def hop(d, h, sub):
        src, dst = (h - 1, h) if d == 0 else ((9 - h) % 8, 8 - h)
        part = pl.ds(sub * rows, rows)
        return pltpu.make_async_remote_copy(
            src_ref=held[src].at[part], dst_ref=held[dst].at[part],
            send_sem=zsend.at[d, h - 1, sub], recv_sem=zrecv.at[d, h - 1, sub],
            device_id=(me, left if d == 0 else right), device_id_type=MESH)

    def used(d, h, sub):
        return h < 4 or (h == 4 and (sub < SUBS // 2) == (d == 0))

    def spread(k):
        block = held[k]

        def pick(i, c):
            base = (peer(i) * 8 + p) * 4
            for s in range(4):
                send[k, i, s] = block[lists[base + s]]
            return c

        lax.fori_loop(0, G, pick, 0)

        def push(i, c):
            pltpu.make_async_remote_copy(
                src_ref=send.at[k, i], dst_ref=land.at[k, me], send_sem=ssem.at[k], recv_sem=rsem.at[k],
                device_id=(peer(i), p), device_id_type=MESH).start()
            return c

        pltpu.make_async_copy(send.at[k, 0], land.at[k, me], rsem.at[k]).start()
        lax.fori_loop(1, G, push, 0)

    for sub in range(SUBS):
        for d in range(2):
            hop(d, 1, sub).start()
    spread(0)
    for h in range(1, 5):
        for sub in range(SUBS):
            for d in range(2):
                if used(d, h, sub):
                    hop(d, h, sub).wait_recv()
                    if used(d, h + 1, sub):
                        hop(d, h + 1, sub).start()
        spread(h)
        if h < 4:
            spread(8 - h)
    for h in range(1, 5):
        for sub in range(SUBS):
            for d in range(2):
                if used(d, h, sub):
                    hop(d, h, sub).wait_send()
    for k in range(8):
        pltpu.make_async_remote_copy(
            src_ref=send.at[k, pl.ds(1, G - 1)], dst_ref=land.at[k, pl.ds(1, G - 1)],
            send_sem=ssem.at[k], recv_sem=rsem.at[k], device_id=(me, right), device_id_type=MESH).wait_send()
        pltpu.make_async_copy(land.at[k], land.at[k], rsem.at[k]).wait()


def gather_boxes(orb, lists, gy, gx):
    G = gy * gx * 2
    norb = orb.shape[0]
    vmem = pl.BlockSpec(memory_space=pltpu.VMEM)
    return pl.pallas_call(
        lambda *refs: gather_kernel(gy, gx, *refs),
        out_shape=jax.ShapeDtypeStruct((8, G, 4, 8, 128), bf16),
        in_specs=[vmem, pl.BlockSpec(memory_space=pltpu.SMEM)],
        out_specs=vmem,
        scratch_shapes=[pltpu.VMEM((norb, 8, 128), bf16)] * 7 + [
            pltpu.VMEM((8, G, 4, 8, 128), bf16),
            pltpu.SemaphoreType.DMA((2, 4, SUBS)),
            pltpu.SemaphoreType.DMA((2, 4, SUBS)),
            pltpu.SemaphoreType.DMA((8,)),
            pltpu.SemaphoreType.DMA((8,)),
        ],
        compiler_params=pltpu.CompilerParams(collective_id=0, has_side_effects=True, vmem_limit_bytes=24 << 20),
        name="gather_boxes",
    )(orb, lists)


def shards(orbitals, box_list, pair_slots, offsets, pair_count):
    planes, orbital_total, row_cells = orbitals.shape
    lists = box_list.reshape(-1)
    orb = orbitals.reshape(planes, orbital_total, 4, 128).transpose(1, 2, 0, 3).reshape(orbital_total, 8, 128)
    land = gather_boxes(orb, lists, 4, 4)
    back = worker_fields(land, pair_slots[0, 0], offsets[0, 0], pair_count[0])
    landed = lax.all_to_all(back.reshape(256, 4, 8, 128), ("grid", "pair"), split_axis=0, concat_axis=0, tiled=True)
    hot = (lists[:, None] == jnp.arange(orbital_total, dtype=jnp.int32)[None, :]).astype(bf16)
    landed = landed.reshape(1024, 4, planes, 128)
    summed = jnp.einsum("ro,rqxc->xoqc", hot, landed, preferred_element_type=f32)
    return summed.reshape(planes, orbital_total, row_cells)


def solution(mesh):
    placed = (
        P("grid", None, "pair"),
        P(),
        P("grid", "pair", None, None),
        P("grid", "pair", None, None),
        P("grid", "pair"),
    )
    return jax.shard_map(
        shards, mesh=mesh, in_specs=placed, out_specs=P("grid", None, "pair"), check_vma=False
    )
```

```python
import math
import numpy as np
import jax
import jax.numpy as jnp
from jax import lax
from jax.experimental import pallas as pl
from jax.experimental.pallas import tpu as pltpu
from jax.sharding import PartitionSpec as P

screening = 0.02
N = 64
CH = 16
W = 256
PITCH = 72
f32, bf16 = jnp.float32, jnp.bfloat16


def tables():
    m = np.arange(N)
    ph = 2.0 * math.pi * ((m[:, None] * m[None, :]) % N) / N
    cas = np.cos(ph) + np.sin(ph)
    perm = np.concatenate([np.arange(0, N, 2), np.arange(1, N, 2)])

    def parts(a):
        a = np.asarray(a, np.float32)
        hi = a.astype(bf16)
        lo = (a - hi.astype(np.float32)).astype(bf16)
        return hi, lo

    def left(a):
        hi, lo = parts(a)
        return np.concatenate([hi, hi, lo], axis=1)

    cx = left(cas[:, perm])
    ux = left(cas[perm, :])
    cf = left(cas[:, perm])
    ci = left(cas[perm, :])
    hi, lo = parts(np.kron(np.eye(4), cas))
    bd = np.concatenate([hi, hi, lo], axis=0)
    e = 2.0 - 2.0 * np.cos(2.0 * math.pi * m / N)
    green = 1.0 / ((screening + e[:, None, None] + e[None, :, None] + e[None, None, :]) * float(N**3))
    g = green.reshape(CH, 4, N, N).transpose(0, 2, 1, 3).reshape(CH, N, W).astype(np.float32)
    return cx, ux, bd, g


def split(v):
    hi = v.astype(bf16)
    lo = (v - hi.astype(f32)).astype(bf16)
    return hi, lo


def mm(a, b):
    return jnp.dot(a, b, preferred_element_type=f32)


def left_mul(table, v):
    hi, lo = split(v)
    return mm(table, jnp.concatenate([hi, lo, hi], axis=0))


def right_mul(v, bd):
    hi, lo = split(v)
    return mm(jnp.concatenate([hi, lo, hi], axis=1), bd)


def pair_kernel(slots, offs, count, land, cx, ux, bd, green, out, box, pad, X, U, F, wh, wl, col):
    GR = 16
    low = lax.broadcasted_iota(jnp.int32, (32, 128), 1) < 64
    zpad = jnp.zeros((4, N, W), bf16)
    for r in (pad, wh, wl):
        r[0:4] = zpad
        r[20:24] = zpad
    col[...] = jnp.zeros(col.shape, f32)
    X[...] = jnp.zeros(X.shape, f32)
    place = lax.axis_index("pair")

    def arrange(s, c):
        def widen(g, c2):
            for k in range(8):
                F[pl.ds(pl.multiple_of(g * PITCH, 8) + 8 * k, 8), :] = land[k, g, s].astype(f32)
            return c2

        lax.fori_loop(0, 32, widen, 0)
        for k in range(8):
            j = (place + k) % 8 * 2
            for jj in range(2):
                for half in range(2):
                    two = [F[pl.ds(8 * k + 4 * jj + 2 * half + xx, 32, stride=PITCH), :] for xx in range(2)]
                    box[s, j + jj, :, half * 128:(half + 1) * 128] = jnp.concatenate(two, axis=0).astype(bf16)
        return c

    lax.fori_loop(0, 4, arrange, 0)

    def pair(k, carry):
        a = slots[k, 0]
        b = slots[k, 1]
        dx, dy, dz = offs[k, 0], offs[k, 1], offs[k, 2]
        t = dy * 64 + dz
        q = (t + 1024) // 256 - 4
        r = t - 256 * q
        rows = lax.broadcasted_iota(jnp.int32, (W, W), 0)
        cols = lax.broadcasted_iota(jnp.int32, (W, W), 1)
        zc = cols % 64 + dz
        okc = (zc >= 0) & (zc < 64)
        one, zero = jnp.float32(1), jnp.float32(0)

        def mask(c):
            return jnp.where(c, one, zero).astype(bf16)

        fwd = jnp.concatenate([mask(okc & (rows == cols + r)), mask(okc & (rows == cols + r - 256))], axis=0)
        zr = rows % 64 + dz
        okr = (zr >= 0) & (zr < 64)
        b0 = mask(okr & (cols == rows + r))
        b1 = mask(okr & (cols == rows + r - 256))
        bwd = jnp.concatenate([b0, b0, b1, b1], axis=0)
        pad[4:20] = box[b]

        def put(j, v):
            for h in range(2):
                for e in range(2):
                    X[j, h, e * 48 + 8:e * 48 + 40, :] = v[e * 32:(e + 1) * 32, h * 128:(h + 1) * 128]

        def moved(j, step):
            halves = []
            for h in range(2):
                both = []
                for e in range(2):
                    n = step + 16 + e
                    both.append(X[j, h, pl.ds(n % 2 * 48 + n // 2, 32), :])
                halves.append(jnp.concatenate(both, axis=0))
            return jnp.concatenate(halves, axis=1)

        def forward(g, c):
            lo_ = g * GR
            src0 = pad[pl.ds(lo_ + 4 + q, GR)].reshape(GR * N, W)
            src1 = pad[pl.ds(lo_ + 5 + q, GR)].reshape(GR * N, W)
            yz = mm(jnp.concatenate([src0, src1], axis=1), fwd).reshape(GR, N, W)
            for i in range(GR):
                put(lo_ + i, yz[i])
            outs = []
            for i in range(GR):
                dens = box[a, lo_ + i].astype(f32) * moved(lo_ + i, dx)
                outs.append(left_mul(cx[...], dens))
            spec = right_mul(jnp.concatenate(outs, axis=0), bd[...])
            for i in range(GR):
                for h in range(2):
                    U[pl.ds(pl.multiple_of((2 * (lo_ + i) + h) * PITCH, 8), N), :] = spec[i * N:(i + 1) * N, h * 128:(h + 1) * 128]
            return c

        lax.fori_loop(0, CH // GR, forward, 0)

        def middle(g, c):
            tops, bots = [], []
            for h in range(2):
                l1 = U[pl.ds(g * 4 + 2 * h, 32, stride=PITCH), :]
                l2 = U[pl.ds(g * 4 + 2 * h + 1, 32, stride=PITCH), :]
                tops.append(jnp.where(low, l1, pltpu.roll(l2, 64, 1)))
                bots.append(jnp.where(low, pltpu.roll(l1, 64, 1), l2))
            v = jnp.concatenate([jnp.concatenate(tops, axis=1), jnp.concatenate(bots, axis=1)], axis=0)
            s = left_mul(cx[...], v) * green[g]
            p = left_mul(ux[...], s)
            for h in range(2):
                x0 = p[:32, h * 128:(h + 1) * 128]
                x1 = p[32:, h * 128:(h + 1) * 128]
                U[pl.ds(g * 4 + 2 * h, 32, stride=PITCH), :] = jnp.where(low, x0, pltpu.roll(x1, 64, 1))
                U[pl.ds(g * 4 + 2 * h + 1, 32, stride=PITCH), :] = jnp.where(low, pltpu.roll(x0, 64, 1), x1)
            return c

        lax.fori_loop(0, CH, middle, 0, unroll=8)

        def inverse(g, c):
            lo_ = g * GR
            outs = []
            for i in range(GR):
                v = jnp.concatenate(
                    [U[pl.ds(pl.multiple_of((2 * (lo_ + i) + h) * PITCH, 8), N), :] for h in range(2)], axis=1)
                outs.append(left_mul(ux[...], v))
            pot = right_mul(jnp.concatenate(outs, axis=0), bd[...]).reshape(GR, N, W)
            for i in range(GR):
                j = lo_ + i
                col[a, j] = col[a, j] - pot[i] * moved(j, dx)
                put(j, -(pot[i] * box[a, j].astype(f32)))
                wh[j + 4], wl[j + 4] = split(moved(j, -dx))
            return c

        lax.fori_loop(0, CH // GR, inverse, 0)

        def back(g, c):
            lo_ = g * GR
            i0 = lo_ + 4 - q
            parts_ = [r_[pl.ds(i, GR)].reshape(GR * N, W) for i in (i0, i0 - 1) for r_ in (wh, wl)]
            u = mm(jnp.concatenate(parts_, axis=1), bwd)
            col[b, pl.ds(lo_, GR)] = col[b, pl.ds(lo_, GR)] + u.reshape(GR, N, W)
            return c

        lax.fori_loop(0, CH // GR, back, 0)
        return carry

    lax.fori_loop(0, count[0], pair, 0)

    def deliver(s, c):
        for k in range(8):
            for jj in range(2):
                for half in range(2):
                    for xx in range(2):
                        F[pl.ds(8 * k + 4 * jj + 2 * half + xx, 32, stride=PITCH), :] = (
                            col[s, 2 * k + jj, xx * 32:(xx + 1) * 32, half * 128:(half + 1) * 128])

        def narrow(g, c2):
            for k in range(8):
                out[g, k, s] = F[pl.ds(pl.multiple_of(g * PITCH, 8) + 8 * k, 8), :].astype(bf16)
            return c2

        lax.fori_loop(0, 32, narrow, 0)
        return c

    lax.fori_loop(0, 4, deliver, 0)


def worker_fields(land, slots, offs, count):
    cx, ux, bd, g = (jnp.asarray(t) for t in tables())
    smem = pl.BlockSpec(memory_space=pltpu.SMEM)
    vmem = pl.BlockSpec(memory_space=pltpu.VMEM)
    return pl.pallas_call(
        pair_kernel,
        out_shape=jax.ShapeDtypeStruct((32, 8, 4, 8, 128), bf16),
        in_specs=[smem] * 3 + [vmem] * 5,
        out_specs=vmem,
        scratch_shapes=[
            pltpu.VMEM((4, CH, N, W), bf16),
            pltpu.VMEM((24, N, W), bf16),
            pltpu.VMEM((CH, 2, 96, 128), f32),
            pltpu.VMEM((32 * PITCH, 128), f32),
            pltpu.VMEM((32 * PITCH, 128), f32),
            pltpu.VMEM((24, N, W), bf16),
            pltpu.VMEM((24, N, W), bf16),
            pltpu.VMEM((4, CH, N, W), f32),
        ],
        compiler_params=pltpu.CompilerParams(vmem_limit_bytes=40 << 20),
        name="pairs",
    )(slots, offs, count, land, cx, ux, bd, g)


MESH = pl.DeviceIdType.MESH
SUBS = 4


def gather_kernel(gy, gx, orb, lists, land, *rest):
    blocks = rest[:7]
    send, zsend, zrecv, ssem, rsem = rest[7:]
    G = gy * gx * 2
    me = lax.axis_index("grid")
    p = lax.axis_index("pair")
    my_y, my_x, my_c = me // (2 * gx), (me // 2) % gx, me % 2
    right, left = (p + 1) % 8, (p + 7) % 8
    held = (orb,) + tuple(blocks)
    rows = orb.shape[0] // SUBS

    def peer(i):
        y = (my_y + i // (2 * gx)) % gy
        x = (my_x + (i // 2) % gx) % gx
        c = (my_c + i) % 2
        return (y * gx + x) * 2 + c

    barrier = pltpu.get_barrier_semaphore()
    pl.semaphore_signal(barrier, inc=1, device_id=(me, right), device_id_type=MESH)
    pl.semaphore_signal(barrier, inc=1, device_id=(me, left), device_id_type=MESH)

    def greet(i, c):
        pl.semaphore_signal(barrier, inc=1, device_id=(peer(i), p), device_id_type=MESH)
        return c

    lax.fori_loop(1, G, greet, 0)

    def hop(d, h, sub):
        src, dst = (h - 1, h) if d == 0 else ((9 - h) % 8, 8 - h)
        part = pl.ds(sub * rows, rows)
        return pltpu.make_async_remote_copy(
            src_ref=held[src].at[part], dst_ref=held[dst].at[part],
            send_sem=zsend.at[d, h - 1, sub], recv_sem=zrecv.at[d, h - 1, sub],
            device_id=(me, left if d == 0 else right), device_id_type=MESH)

    def used(d, h, sub):
        return h < 4 or (h == 4 and (sub < SUBS // 2) == (d == 0))

    def pick(k):
        block = held[k]

        def some(t, c):
            for i in range(4):
                g = t * 4 + i
                for s in range(4):
                    send[k, g, s] = block[lists[(g * 8 + p) * 4 + s]]
            return c

        lax.fori_loop(0, G // 4, some, 0)

    def push(k):
        def one(i, c):
            g = peer(i)
            pltpu.make_async_remote_copy(
                src_ref=send.at[k, g], dst_ref=land.at[k, me], send_sem=ssem.at[k], recv_sem=rsem.at[k],
                device_id=(g, p), device_id_type=MESH).start()
            return c

        pltpu.make_async_copy(send.at[k, me], land.at[k, me], rsem.at[k]).start()
        lax.fori_loop(1, G, one, 0)

    pick(0)
    pl.semaphore_wait(barrier, G + 1)
    for sub in range(SUBS):
        for d in range(2):
            hop(d, 1, sub).start()
    push(0)
    for h in range(1, 5):
        for sub in range(SUBS):
            for d in range(2):
                if used(d, h, sub):
                    hop(d, h, sub).wait_recv()
                    if used(d, h + 1, sub):
                        hop(d, h + 1, sub).start()
        for k in (h, 8 - h) if h < 4 else (h,):
            pick(k)
            push(k)
    for h in range(1, 5):
        for sub in range(SUBS):
            for d in range(2):
                if used(d, h, sub):
                    hop(d, h, sub).wait_send()
    for k in range(8):
        pltpu.make_async_remote_copy(
            src_ref=send.at[k, pl.ds(1, G - 1)], dst_ref=land.at[k, pl.ds(1, G - 1)],
            send_sem=ssem.at[k], recv_sem=rsem.at[k], device_id=(me, right), device_id_type=MESH).wait_send()
        pltpu.make_async_copy(land.at[k], land.at[k], rsem.at[k]).wait()


def gather_boxes(orb, lists, gy, gx):
    G = gy * gx * 2
    norb = orb.shape[0]
    vmem = pl.BlockSpec(memory_space=pltpu.VMEM)
    return pl.pallas_call(
        lambda *refs: gather_kernel(gy, gx, *refs),
        out_shape=jax.ShapeDtypeStruct((8, G, 4, 8, 128), bf16),
        in_specs=[vmem, pl.BlockSpec(memory_space=pltpu.SMEM)],
        out_specs=vmem,
        scratch_shapes=[pltpu.VMEM((norb, 8, 128), bf16)] * 7 + [
            pltpu.VMEM((8, G, 4, 8, 128), bf16),
            pltpu.SemaphoreType.DMA((2, 4, SUBS)),
            pltpu.SemaphoreType.DMA((2, 4, SUBS)),
            pltpu.SemaphoreType.DMA((8,)),
            pltpu.SemaphoreType.DMA((8,)),
        ],
        compiler_params=pltpu.CompilerParams(collective_id=0, has_side_effects=True, vmem_limit_bytes=24 << 20),
        name="gather_boxes",
    )(orb, lists)


def shards(orbitals, box_list, pair_slots, offsets, pair_count):
    planes, orbital_total, row_cells = orbitals.shape
    lists = box_list.reshape(-1)
    orb = orbitals.reshape(planes, orbital_total, 4, 128).transpose(1, 2, 0, 3).reshape(orbital_total, 8, 128)
    land = gather_boxes(orb, lists, 4, 4)
    back = worker_fields(land, pair_slots[0, 0], offsets[0, 0], pair_count[0])
    landed = lax.all_to_all(back.reshape(256, 4, 8, 128), ("grid", "pair"), split_axis=0, concat_axis=0, tiled=True)
    hot = (lists[:, None] == jnp.arange(orbital_total, dtype=jnp.int32)[None, :]).astype(bf16)
    landed = landed.reshape(1024, 4, planes, 128)
    summed = jnp.einsum("ro,rqxc->xoqc", hot, landed, preferred_element_type=f32)
    return summed.reshape(planes, orbital_total, row_cells)


def solution(mesh):
    placed = (
        P("grid", None, "pair"),
        P(),
        P("grid", "pair", None, None),
        P("grid", "pair", None, None),
        P("grid", "pair"),
    )
    return jax.shard_map(
        shards, mesh=mesh, in_specs=placed, out_specs=P("grid", None, "pair"), check_vma=False
    )
```

```python
import math
import numpy as np
import jax
import jax.numpy as jnp
from jax import lax
from jax.experimental import pallas as pl
from jax.experimental.pallas import tpu as pltpu
from jax.sharding import PartitionSpec as P

screening = 0.02
N = 64
CH = 16
W = 256
PITCH = 72
PITCH2 = 24
f32, bf16 = jnp.float32, jnp.bfloat16


def tables():
    m = np.arange(N)
    ph = 2.0 * math.pi * ((m[:, None] * m[None, :]) % N) / N
    cas = np.cos(ph) + np.sin(ph)
    perm = np.concatenate([np.arange(0, N, 2), np.arange(1, N, 2)])

    def parts(a):
        a = np.asarray(a, np.float32)
        hi = a.astype(bf16)
        lo = (a - hi.astype(np.float32)).astype(bf16)
        return hi, lo

    def left(a):
        hi, lo = parts(a)
        return np.concatenate([hi, hi, lo], axis=1)

    cx = left(cas[:, perm])
    ux = left(cas[perm, :])
    cf = left(cas[:, perm])
    ci = left(cas[perm, :])
    hi, lo = parts(np.kron(np.eye(4), cas))
    bd = np.concatenate([hi, hi, lo], axis=0)
    e = 2.0 - 2.0 * np.cos(2.0 * math.pi * m / N)
    green = 1.0 / ((screening + e[:, None, None] + e[None, :, None] + e[None, None, :]) * float(N**3))
    g = green.reshape(CH, 4, N, N).transpose(0, 2, 1, 3).reshape(CH, N, W).astype(np.float32)
    return cx, ux, bd, g


def split(v):
    hi = v.astype(bf16)
    lo = (v - hi.astype(f32)).astype(bf16)
    return hi, lo


def mm(a, b):
    return jnp.dot(a, b, preferred_element_type=f32)


def left_mul(table, v):
    hi, lo = split(v)
    return mm(table, jnp.concatenate([hi, lo, hi], axis=0))


def right_mul(v, bd):
    hi, lo = split(v)
    return mm(jnp.concatenate([hi, lo, hi], axis=1), bd)


def pair_kernel(slots, offs, count, land, cx, ux, bd, green, out, box, pad, X, U, F, wh, wl, col):
    GR = 16
    low = lax.broadcasted_iota(jnp.int32, (32, 128), 1) < 64
    zpad = jnp.zeros((4, N, W), bf16)
    for r in (pad, wh, wl):
        r[0:4] = zpad
        r[20:24] = zpad
    col[...] = jnp.zeros(col.shape, f32)
    X[...] = jnp.zeros(X.shape, f32)
    place = lax.axis_index("pair")

    def arrange(s, c):
        def widen(t, c2):
            for i in range(4):
                g = t * 4 + i
                for k in range(8):
                    F[pl.ds(pl.multiple_of(g * PITCH, 8) + 8 * k, 8), :] = land[k, g, s].astype(f32)
            return c2

        lax.fori_loop(0, 8, widen, 0)
        for k in range(8):
            j = (place + k) % 8 * 2
            for jj in range(2):
                for half in range(2):
                    two = [F[pl.ds(8 * k + 4 * jj + 2 * half + xx, 32, stride=PITCH), :] for xx in range(2)]
                    box[s, j + jj, :, half * 128:(half + 1) * 128] = jnp.concatenate(two, axis=0).astype(bf16)
        return c

    lax.fori_loop(0, 4, arrange, 0)

    def pair(k, carry):
        a = slots[0, k]
        b = slots[1, k]
        dx, dy, dz = offs[0, 0, k], offs[1, 0, k], offs[2, 0, k]
        t = dy * 64 + dz
        q = (t + 1024) // 256 - 4
        r = t - 256 * q
        rows = lax.broadcasted_iota(jnp.int32, (W, W), 0)
        cols = lax.broadcasted_iota(jnp.int32, (W, W), 1)
        zc = cols % 64 + dz
        okc = (zc >= 0) & (zc < 64)
        one, zero = jnp.float32(1), jnp.float32(0)

        def mask(c):
            return jnp.where(c, one, zero).astype(bf16)

        fwd = jnp.concatenate([mask(okc & (rows == cols + r)), mask(okc & (rows == cols + r - 256))], axis=0)
        zr = rows % 64 + dz
        okr = (zr >= 0) & (zr < 64)
        b0 = mask(okr & (cols == rows + r))
        b1 = mask(okr & (cols == rows + r - 256))
        bwd = jnp.concatenate([b0, b0, b1, b1], axis=0)
        pad[4:20] = box[b]

        def put(j, v):
            for h in range(2):
                for e in range(2):
                    X[j, h, e * 48 + 8:e * 48 + 40, :] = v[e * 32:(e + 1) * 32, h * 128:(h + 1) * 128]

        def moved(j, step):
            halves = []
            for h in range(2):
                both = []
                for e in range(2):
                    n = step + 16 + e
                    both.append(X[j, h, pl.ds(n % 2 * 48 + n // 2, 32), :])
                halves.append(jnp.concatenate(both, axis=0))
            return jnp.concatenate(halves, axis=1)

        def forward(g, c):
            lo_ = g * GR
            src0 = pad[pl.ds(lo_ + 4 + q, GR)].reshape(GR * N, W)
            src1 = pad[pl.ds(lo_ + 5 + q, GR)].reshape(GR * N, W)
            yz = mm(jnp.concatenate([src0, src1], axis=1), fwd).reshape(GR, N, W)
            for i in range(GR):
                put(lo_ + i, yz[i])
            outs = []
            for i in range(GR):
                dens = box[a, lo_ + i].astype(f32) * moved(lo_ + i, dx)
                outs.append(left_mul(cx[...], dens))
            spec = right_mul(jnp.concatenate(outs, axis=0), bd[...])
            for i in range(GR):
                for h in range(2):
                    U[pl.ds(pl.multiple_of((2 * (lo_ + i) + h) * PITCH, 8), N), :] = spec[i * N:(i + 1) * N, h * 128:(h + 1) * 128]
            return c

        lax.fori_loop(0, CH // GR, forward, 0)

        def middle(g, c):
            tops, bots = [], []
            for h in range(2):
                l1 = U[pl.ds(g * 4 + 2 * h, 32, stride=PITCH), :]
                l2 = U[pl.ds(g * 4 + 2 * h + 1, 32, stride=PITCH), :]
                tops.append(jnp.where(low, l1, pltpu.roll(l2, 64, 1)))
                bots.append(jnp.where(low, pltpu.roll(l1, 64, 1), l2))
            v = jnp.concatenate([jnp.concatenate(tops, axis=1), jnp.concatenate(bots, axis=1)], axis=0)
            s = left_mul(cx[...], v) * green[g]
            p = left_mul(ux[...], s)
            for h in range(2):
                x0 = p[:32, h * 128:(h + 1) * 128]
                x1 = p[32:, h * 128:(h + 1) * 128]
                U[pl.ds(g * 4 + 2 * h, 32, stride=PITCH), :] = jnp.where(low, x0, pltpu.roll(x1, 64, 1))
                U[pl.ds(g * 4 + 2 * h + 1, 32, stride=PITCH), :] = jnp.where(low, pltpu.roll(x0, 64, 1), x1)
            return c

        lax.fori_loop(0, CH, middle, 0, unroll=8)

        def inverse(g, c):
            lo_ = g * GR
            outs = []
            for i in range(GR):
                v = jnp.concatenate(
                    [U[pl.ds(pl.multiple_of((2 * (lo_ + i) + h) * PITCH, 8), N), :] for h in range(2)], axis=1)
                outs.append(left_mul(ux[...], v))
            pot = right_mul(jnp.concatenate(outs, axis=0), bd[...]).reshape(GR, N, W)
            for i in range(GR):
                j = lo_ + i
                col[a, j] = col[a, j] - pot[i] * moved(j, dx)
                put(j, -(pot[i] * box[a, j].astype(f32)))
                wh[j + 4], wl[j + 4] = split(moved(j, -dx))
            return c

        lax.fori_loop(0, CH // GR, inverse, 0)

        def back(g, c):
            lo_ = g * GR
            i0 = lo_ + 4 - q
            parts_ = [r_[pl.ds(i, GR)].reshape(GR * N, W) for i in (i0, i0 - 1) for r_ in (wh, wl)]
            u = mm(jnp.concatenate(parts_, axis=1), bwd)
            col[b, pl.ds(lo_, GR)] = col[b, pl.ds(lo_, GR)] + u.reshape(GR, N, W)
            return c

        lax.fori_loop(0, CH // GR, back, 0)
        return carry

    lax.fori_loop(0, count[0, 0], pair, 0)

    def deliver(k, c):
        j = (place + k) % 8 * 2
        for s in range(4):
            for jj in range(2):
                for half in range(2):
                    for xx in range(2):
                        F[pl.ds(32 * PITCH2 * half + 4 * s + 2 * jj + xx, 32, stride=PITCH2), :] = (
                            col[s, j + jj, xx * 32:(xx + 1) * 32, half * 128:(half + 1) * 128])

        def narrow(t, c2):
            for i in range(4):
                g = t * 4 + i
                for half in range(2):
                    out[k, g, half] = F[pl.ds(pl.multiple_of((half * 32 + g) * PITCH2, 8), 16), :].astype(bf16)
            return c2

        lax.fori_loop(0, 8, narrow, 0)
        return c

    lax.fori_loop(0, 8, deliver, 0)


def worker_fields(land, slots, offs, count):
    cx, ux, bd, g = (jnp.asarray(t) for t in tables())
    smem = pl.BlockSpec(memory_space=pltpu.SMEM)
    vmem = pl.BlockSpec(memory_space=pltpu.VMEM)
    return pl.pallas_call(
        pair_kernel,
        out_shape=jax.ShapeDtypeStruct((8, 32, 2, 16, 128), bf16),
        in_specs=[smem] * 3 + [vmem] * 5,
        out_specs=vmem,
        scratch_shapes=[
            pltpu.VMEM((4, CH, N, W), bf16),
            pltpu.VMEM((24, N, W), bf16),
            pltpu.VMEM((CH, 2, 96, 128), f32),
            pltpu.VMEM((32 * PITCH, 128), f32),
            pltpu.VMEM((32 * PITCH, 128), f32),
            pltpu.VMEM((24, N, W), bf16),
            pltpu.VMEM((24, N, W), bf16),
            pltpu.VMEM((4, CH, N, W), f32),
        ],
        compiler_params=pltpu.CompilerParams(vmem_limit_bytes=28 << 20),
        name="pairs",
    )(slots, offs, count, land, cx, ux, bd, g)


MESH = pl.DeviceIdType.MESH
SUBS = 4


def gather_kernel(gy, gx, orb, lists, land, *rest):
    blocks = rest[:8]
    wide, send, zsend, zrecv, ssem, rsem = rest[8:]
    G = gy * gx * 2
    me = lax.axis_index("grid")
    p = lax.axis_index("pair")
    my_y, my_x, my_c = me // (2 * gx), (me // 2) % gx, me % 2
    right, left = (p + 1) % 8, (p + 7) % 8
    held = blocks
    norb = orb.shape[1]
    pitch = norb + 8
    rows = norb // SUBS
    batch = min(4, G)

    def peer(i):
        y = (my_y + i // (2 * gx)) % gy
        x = (my_x + (i // 2) % gx) % gx
        c = (my_c + i) % 2
        return (y * gx + x) * 2 + c

    barrier = pltpu.get_barrier_semaphore()
    pl.semaphore_signal(barrier, inc=1, device_id=(me, right), device_id_type=MESH)
    pl.semaphore_signal(barrier, inc=1, device_id=(me, left), device_id_type=MESH)

    def greet(i, c):
        pl.semaphore_signal(barrier, inc=1, device_id=(peer(i), p), device_id_type=MESH)
        return c

    lax.fori_loop(1, G, greet, 0)

    def hop(d, h, sub):
        src, dst = (h - 1, h) if d == 0 else ((9 - h) % 8, 8 - h)
        part = pl.ds(sub * rows, rows)
        return pltpu.make_async_remote_copy(
            src_ref=held[src].at[part], dst_ref=held[dst].at[part],
            send_sem=zsend.at[d, h - 1, sub], recv_sem=zrecv.at[d, h - 1, sub],
            device_id=(me, left if d == 0 else right), device_id_type=MESH)

    def used(d, h, sub):
        return h < 4 or (h == 4 and (sub < SUBS // 2) == (d == 0))

    def pick(k):
        block = held[k]

        def some(t, c):
            for i in range(batch):
                g = t * batch + i
                for s in range(4):
                    send[k, g, s] = block[lists[p, s, g]]
            return c

        lax.fori_loop(0, G // batch, some, 0)

    def push(k):
        def one(i, c):
            g = peer(i)
            pltpu.make_async_remote_copy(
                src_ref=send.at[k, g], dst_ref=land.at[k, me], send_sem=ssem.at[k], recv_sem=rsem.at[k],
                device_id=(g, p), device_id_type=MESH).start()
            return c

        pltpu.make_async_copy(send.at[k, me], land.at[k, me], rsem.at[k]).start()
        lax.fori_loop(1, G, one, 0)

    for jj in range(2):
        for half in range(2):
            for xx in range(2):
                r = 4 * jj + 2 * half + xx
                lane = jj * 256 + half * 128
                wide[r * pitch:r * pitch + norb, :] = orb[xx, :, lane:lane + 128].astype(f32)

    def regroup(t, c):
        for i in range(8):
            o = t * 8 + i
            held[0][o] = wide[pl.ds(o, 8, stride=pitch), :].astype(bf16)
        return c

    lax.fori_loop(0, norb // 8, regroup, 0)
    pick(0)
    pl.semaphore_wait(barrier, G + 1)
    for sub in range(SUBS):
        for d in range(2):
            hop(d, 1, sub).start()
    push(0)
    for h in range(1, 5):
        for sub in range(SUBS):
            for d in range(2):
                if used(d, h, sub):
                    hop(d, h, sub).wait_recv()
                    if used(d, h + 1, sub):
                        hop(d, h + 1, sub).start()
        for k in (h, 8 - h) if h < 4 else (h,):
            pick(k)
            push(k)
    for h in range(1, 5):
        for sub in range(SUBS):
            for d in range(2):
                if used(d, h, sub):
                    hop(d, h, sub).wait_send()
    for k in range(8):
        pltpu.make_async_remote_copy(
            src_ref=send.at[k, pl.ds(1, G - 1)], dst_ref=land.at[k, pl.ds(1, G - 1)],
            send_sem=ssem.at[k], recv_sem=rsem.at[k], device_id=(me, right), device_id_type=MESH).wait_send()
        pltpu.make_async_copy(land.at[k], land.at[k], rsem.at[k]).wait()


def gather_boxes(orb, lists, gy, gx):
    G = gy * gx * 2
    norb = orb.shape[1]
    vmem = pl.BlockSpec(memory_space=pltpu.VMEM)
    return pl.pallas_call(
        lambda *refs: gather_kernel(gy, gx, *refs),
        out_shape=jax.ShapeDtypeStruct((8, G, 4, 8, 128), bf16),
        in_specs=[vmem, pl.BlockSpec(memory_space=pltpu.SMEM)],
        out_specs=vmem,
        scratch_shapes=[pltpu.VMEM((norb, 8, 128), bf16)] * 8 + [
            pltpu.VMEM((8 * (norb + 8), 128), f32),
            pltpu.VMEM((8, G, 4, 8, 128), bf16),
            pltpu.SemaphoreType.DMA((2, 4, SUBS)),
            pltpu.SemaphoreType.DMA((2, 4, SUBS)),
            pltpu.SemaphoreType.DMA((8,)),
            pltpu.SemaphoreType.DMA((8,)),
        ],
        compiler_params=pltpu.CompilerParams(collective_id=0, has_side_effects=True, vmem_limit_bytes=12 << 20),
        name="gather_boxes",
    )(orb, lists)


ORDER = ((4, None), (3, None), (5, None), (2, None), (6, None), (1, None), (7, None), (0, None))
NF, NS = 3, 5


def collect_kernel(gy, gx, norb, fields, lists, out, keys, rows, bufa, bufb, bufc, bufd, sumc, sumd, hot, hotc,
                   ssem, rsem, zsend, zrecv):
    G = gy * gx * 2
    HG = G // 2
    K = G * 16
    R = 4 * norb
    me = lax.axis_index("grid")
    p = lax.axis_index("pair")
    my_y, my_x, my_c = me // (2 * gx), (me // 2) % gx, me % 2
    toward = ((p + 1) % 8, (p + 7) % 8)

    def peer(i):
        y = (my_y + i // (2 * gx)) % gy
        x = (my_x + (i // 2) % gx) % gx
        c = (my_c + i) % 2
        return (y * gx + x) * 2 + c

    barrier = pltpu.get_barrier_semaphore()
    for z in toward:
        pl.semaphore_signal(barrier, inc=1, device_id=(me, z), device_id_type=MESH)

    def greet(i, c):
        pl.semaphore_signal(barrier, inc=1, device_id=(peer(i), p), device_id_type=MESH)
        return c

    lax.fori_loop(1, G, greet, 0)

    col_g = lax.broadcasted_iota(jnp.int32, (G, K), 1)
    row_g = lax.broadcasted_iota(jnp.int32, (G, K), 0)
    all_keys = ((lax.broadcasted_iota(jnp.int32, (8, K), 1) % 4) * norb).astype(f32)
    for s in range(4):
        pattern = (col_g // 16 == row_g) & (col_g // 4 % 4 == s)
        pattern = jnp.where(pattern, jnp.float32(1), jnp.float32(0)).astype(bf16)
        all_keys = all_keys + mm(lists[:, s, :].astype(f32).astype(bf16), pattern)
    keys[...] = all_keys.astype(jnp.int32)

    def choose(q, lo, n):
        key = keys[pl.ds(q, 1), lo:lo + n]
        rowid = lax.broadcasted_iota(jnp.int32, (R, n), 0)
        return jnp.where(rowid == key, jnp.float32(1), jnp.float32(0)).astype(bf16)

    hot[...] = choose(p, 0, K)
    pl.semaphore_wait(barrier, G + 1)

    def view(ref, k, g, h):
        return ref.at[k, g] if h is None else ref.at[k, g, h]

    def slot(k, h):
        return k

    def spread(k, h=None):
        sem = slot(k, h)
        pltpu.make_async_copy(view(fields, k, me, h), view(rows, k, me, h), rsem.at[sem]).start()

        def push(i, c):
            g = peer(i)
            pltpu.make_async_remote_copy(
                src_ref=view(fields, k, g, h), dst_ref=view(rows, k, me, h), send_sem=ssem.at[sem],
                recv_sem=rsem.at[sem], device_id=(g, p), device_id_type=MESH).start()
            return c

        lax.fori_loop(1, G, push, 0)

    def landed(k, h=None):
        part = view(rows, k, slice(None), h)
        pltpu.make_async_copy(part, part, rsem.at[slot(k, h)]).wait()

    def hop(d, stage, h):
        if stage == 0:
            src, dst = rows.at[4, pl.ds(d * HG, HG), h], bufa.at[d, h]
        elif stage == 1:
            src, dst = rows.at[(3, 5)[d], :, h], bufb.at[d, h, pl.ds(0, G)]
        elif stage == 2:
            src, dst = bufa.at[d, h], bufb.at[d, h, pl.ds(G, HG)]
        elif stage == 3:
            src, dst = sumc.at[d, h], bufc.at[d, h]
        else:
            src, dst = sumd.at[d, h], bufd.at[d, h]
        return pltpu.make_async_remote_copy(
            src_ref=src, dst_ref=dst, send_sem=zsend.at[d, stage, h], recv_sem=zrecv.at[d, stage, h],
            device_id=(me, toward[d]), device_id_type=MESH)

    def own(k, h):
        return mm(hot[...], rows[k, :, h].reshape(K, 128))

    for k, h in ORDER[:NF]:
        spread(k, h)
    landed(4)
    for h in range(2):
        for d in range(2):
            hop(d, 0, h).start()
    for k, h in ORDER[NF:NS]:
        spread(k, h)
    for d in range(2):
        q1, q2 = ((p + 7) % 8, (p + 6) % 8) if d == 0 else ((p + 1) % 8, (p + 2) % 8)
        hotc[d, :, 0:K] = choose(q1, 0, K)
        hotc[d, :, K:K + K // 2] = choose(q2, d * (K // 2), K // 2)
    for h in range(2):
        for d in range(2):
            if h == 0:
                landed((3, 5)[d])
            hop(d, 1, h).start()
            hop(d, 0, h).wait_recv()
            hop(d, 2, h).start()
    for k, h in ORDER[NS:]:
        spread(k, h)
    landed(2)
    landed(6)
    for h in range(2):
        for d in range(2):
            hop(d, 1, h).wait_recv()
            hop(d, 2, h).wait_recv()
            sumc[d, h] = own((2, 6)[d], h) + mm(hotc[d], bufb[d, h].reshape(K + K // 2, 128))
            hop(d, 3, h).start()
    landed(1)
    landed(7)
    landed(0)
    mine = [own(0, h) for h in range(2)]
    for h in range(2):
        for d in range(2):
            part = own((1, 7)[d], h)
            hop(d, 3, h).wait_recv()
            sumd[d, h] = (part + bufc[d, h]).astype(bf16)
            hop(d, 4, h).start()
    for h in range(2):
        for d in range(2):
            hop(d, 4, h).wait_recv()
        total = mine[h] + bufd[0, h].astype(f32) + bufd[1, h].astype(f32)
        for jj in range(2):
            for xx in range(2):
                i = jj * 2 + xx
                out[xx, :, jj * 256 + h * 128:jj * 256 + (h + 1) * 128] = total[i * norb:(i + 1) * norb]
    for d in range(2):
        for stage in range(5):
            for h in range(2):
                hop(d, stage, h).wait_send()
    for k, h in ORDER:
        many = pl.ds(1, G - 1)
        pltpu.make_async_remote_copy(
            src_ref=view(fields, k, many, h), dst_ref=view(rows, k, many, h), send_sem=ssem.at[slot(k, h)],
            recv_sem=rsem.at[slot(k, h)], device_id=(me, toward[0]), device_id_type=MESH).wait_send()


def collect_fields(fields, lists, norb, gy, gx):
    G = gy * gx * 2
    vmem = pl.BlockSpec(memory_space=pltpu.VMEM)
    sums = pltpu.VMEM((2, 2, 4 * norb, 128), f32)
    last = pltpu.VMEM((2, 2, 4 * norb, 128), bf16)
    return pl.pallas_call(
        lambda *refs: collect_kernel(gy, gx, norb, *refs),
        out_shape=jax.ShapeDtypeStruct((2, norb, 512), f32),
        in_specs=[vmem, vmem],
        out_specs=vmem,
        scratch_shapes=[
            pltpu.VMEM((8, G * 16), jnp.int32),
            pltpu.VMEM((8, G, 2, 16, 128), bf16),
            pltpu.VMEM((2, 2, G // 2, 16, 128), bf16),
            pltpu.VMEM((2, 2, G + G // 2, 16, 128), bf16),
            sums, last, sums, last,
            pltpu.VMEM((4 * norb, G * 16), bf16),
            pltpu.VMEM((2, 4 * norb, G * 24), bf16),
            pltpu.SemaphoreType.DMA((10,)),
            pltpu.SemaphoreType.DMA((10,)),
            pltpu.SemaphoreType.DMA((2, 5, 2)),
            pltpu.SemaphoreType.DMA((2, 5, 2)),
        ],
        compiler_params=pltpu.CompilerParams(collective_id=1, has_side_effects=True, vmem_limit_bytes=18 << 20),
        name="collect_fields",
    )(fields, lists)


def shards(orbitals, box_list, pair_slots, offsets, pair_count):
    lists = jnp.transpose(box_list, (1, 2, 0))
    slots = jnp.transpose(pair_slots, (0, 1, 3, 2)).reshape(2, 4)
    offs = jnp.transpose(offsets, (0, 3, 1, 2)).reshape(3, 1, 4)
    land = gather_boxes(orbitals, lists, 4, 4)
    fields = worker_fields(land, slots, offs, pair_count)
    return collect_fields(fields, lists, orbitals.shape[1], 4, 4)


def solution(mesh):
    placed = (
        P("grid", None, "pair"),
        P(),
        P("grid", "pair", None, None),
        P("grid", "pair", None, None),
        P("grid", "pair"),
    )
    return jax.shard_map(
        shards, mesh=mesh, in_specs=placed, out_specs=P("grid", None, "pair"), check_vma=False
    )
```

```python
import math
import numpy as np
import jax
import jax.numpy as jnp
from jax import lax
from jax.experimental import pallas as pl
from jax.experimental.pallas import tpu as pltpu
from jax.sharding import PartitionSpec as P

screening = 0.02
N = 64
CH = 16
W = 256
PITCH = 68
PITCH2 = 20
f32, bf16 = jnp.float32, jnp.bfloat16


def tables():
    m = np.arange(N)
    ph = 2.0 * math.pi * ((m[:, None] * m[None, :]) % N) / N
    cas = np.cos(ph) + np.sin(ph)
    perm = np.concatenate([np.arange(0, N, 2), np.arange(1, N, 2)])

    def parts(a):
        a = np.asarray(a, np.float32)
        hi = a.astype(bf16)
        lo = (a - hi.astype(np.float32)).astype(bf16)
        return hi, lo

    def left(a):
        hi, lo = parts(a)
        return np.concatenate([hi, hi, lo], axis=1)

    cx = left(cas[:, perm])
    ux = left(cas[perm, :])
    cf = left(cas[:, perm])
    ci = left(cas[perm, :])
    hi, lo = parts(np.kron(np.eye(4), cas))
    bd = np.concatenate([hi, hi, lo], axis=0)
    e = 2.0 - 2.0 * np.cos(2.0 * math.pi * m / N)
    green = 1.0 / ((screening + e[:, None, None] + e[None, :, None] + e[None, None, :]) * float(N**3))
    g = green.reshape(CH, 4, N, N).transpose(0, 2, 1, 3).reshape(CH, N, W).astype(np.float32)
    return cx, ux, bd, g


def split(v):
    hi = v.astype(bf16)
    lo = (v - hi.astype(f32)).astype(bf16)
    return hi, lo


def mm(a, b):
    return jnp.dot(a, b, preferred_element_type=f32)


def left_mul(table, v):
    hi, lo = split(v)
    return mm(table, jnp.concatenate([hi, lo, hi], axis=0))


def right_mul(v, bd):
    hi, lo = split(v)
    return mm(jnp.concatenate([hi, lo, hi], axis=1), bd)


def pair_kernel(slots, offs, count, land, cx, ux, bd, green, out, box, S, SH, U, F, col):
    low = lax.broadcasted_iota(jnp.int32, (32, 128), 1) < 64
    lane = lax.broadcasted_iota(jnp.int32, (N, 128), 1)
    for r in (slice(0, 6), slice(38, 44)):
        S[r] = jnp.zeros((6, 96, 128), f32)
    for r in (0, 40, 48, 88):
        S[6:38, r:r + 8, :] = jnp.zeros((32, 8, 128), f32)
    col[...] = jnp.zeros(col.shape, f32)
    place = lax.axis_index("pair")

    def arrange(s, c):
        def widen(t, c2):
            for i in range(4):
                g = t * 4 + i
                for k in range(8):
                    F[pl.ds(pl.multiple_of(g * PITCH, 4) + 8 * k, 8), :] = land[k, g, s].astype(f32)
            return c2

        lax.fori_loop(0, 8, widen, 0)
        for k in range(8):
            j = (place + k) % 8 * 2
            for jj in range(2):
                for half in range(2):
                    two = [F[pl.ds(8 * k + 4 * jj + 2 * half + xx, 32, stride=PITCH), :] for xx in range(2)]
                    box[s, j + jj, :, half * 128:(half + 1) * 128] = jnp.concatenate(two, axis=0).astype(bf16)
        return c

    lax.fori_loop(0, 4, arrange, 0)

    def pair(k, carry):
        a = slots[0, k]
        b = slots[1, k]
        dx, dy, dz = offs[0, 0, k], offs[1, 0, k], offs[2, 0, k]
        t = dy * 64 + dz
        q = (t + 1024) // 128 - 8
        r = t - 128 * q
        z = lane % 64
        inside = (z + dz >= 0) & (z + dz < 64)
        inside_back = (z - dz >= 0) & (z - dz < 64)

        def put(j, v):
            for h in range(2):
                for e in range(2):
                    S[6 + 2 * j + h, e * 48 + 8:e * 48 + 40, :] = v[e * 32:(e + 1) * 32, h * 128:(h + 1) * 128]

        def fetch(tile, step, turn):
            both = []
            for e in range(2):
                n = step + 16 + e
                both.append(S[tile, pl.ds(n % 2 * 48 + n // 2, 32), :])
            return pltpu.roll(jnp.concatenate(both, axis=0), turn, 1)

        for j in range(CH):
            put(j, box[b, j].astype(f32))
        turn = (128 - r) % 128
        here = fetch(6 + q, dx, turn)
        for T in range(2 * CH):
            then = fetch(7 + T + q, dx, turn)
            SH[T] = jnp.where(inside, jnp.where(lane < 128 - r, here, then), jnp.float32(0))
            here = then

        outs = []
        for j in range(CH):
            moved = jnp.concatenate([SH[2 * j], SH[2 * j + 1]], axis=1)
            outs.append(left_mul(cx[...], box[a, j].astype(f32) * moved))
        spec = right_mul(jnp.concatenate(outs, axis=0), bd[...])
        for j in range(CH):
            for h in range(2):
                U[(2 * j + h) * PITCH:(2 * j + h) * PITCH + N, :] = spec[j * N:(j + 1) * N, h * 128:(h + 1) * 128]

        def middle(g, c):
            tops, bots = [], []
            for h in range(2):
                l1 = U[pl.ds(g * 4 + 2 * h, 32, stride=PITCH), :]
                l2 = U[pl.ds(g * 4 + 2 * h + 1, 32, stride=PITCH), :]
                tops.append(jnp.where(low, l1, pltpu.roll(l2, 64, 1)))
                bots.append(jnp.where(low, pltpu.roll(l1, 64, 1), l2))
            v = jnp.concatenate([jnp.concatenate(tops, axis=1), jnp.concatenate(bots, axis=1)], axis=0)
            s = left_mul(cx[...], v) * green[g]
            p = left_mul(ux[...], s)
            for h in range(2):
                x0 = p[:32, h * 128:(h + 1) * 128]
                x1 = p[32:, h * 128:(h + 1) * 128]
                U[pl.ds(g * 4 + 2 * h, 32, stride=PITCH), :] = jnp.where(low, x0, pltpu.roll(x1, 64, 1))
                U[pl.ds(g * 4 + 2 * h + 1, 32, stride=PITCH), :] = jnp.where(low, pltpu.roll(x0, 64, 1), x1)
            return c

        lax.fori_loop(0, CH, middle, 0, unroll=8)

        outs = []
        for j in range(CH):
            v = jnp.concatenate([U[(2 * j + h) * PITCH:(2 * j + h) * PITCH + N, :] for h in range(2)], axis=1)
            outs.append(left_mul(ux[...], v))
        pot = right_mul(jnp.concatenate(outs, axis=0), bd[...]).reshape(CH, N, W)
        for j in range(CH):
            moved = jnp.concatenate([SH[2 * j], SH[2 * j + 1]], axis=1)
            col[a, j] = col[a, j] - pot[j] * moved
            put(j, -(pot[j] * box[a, j].astype(f32)))

        here = fetch(5 - q, -dx, r)
        for T in range(2 * CH):
            then = fetch(6 + T - q, -dx, r)
            u = jnp.where(inside_back, jnp.where(lane < r, here, then), jnp.float32(0))
            part = slice(T % 2 * 128, T % 2 * 128 + 128)
            col[b, T // 2, :, part] = col[b, T // 2, :, part] + u
            here = then
        return carry

    lax.fori_loop(0, count[0, 0], pair, 0)

    def deliver(k, c):
        j = (place + k) % 8 * 2
        for s in range(4):
            for jj in range(2):
                for half in range(2):
                    for xx in range(2):
                        F[pl.ds(32 * PITCH2 * half + 4 * s + 2 * jj + xx, 32, stride=PITCH2), :] = (
                            col[s, j + jj, xx * 32:(xx + 1) * 32, half * 128:(half + 1) * 128])

        def narrow(t, c2):
            for i in range(4):
                g = t * 4 + i
                for half in range(2):
                    out[k, g, half] = F[pl.ds(pl.multiple_of((half * 32 + g) * PITCH2, 4), 16), :].astype(bf16)
            return c2

        lax.fori_loop(0, 8, narrow, 0)
        return c

    lax.fori_loop(0, 8, deliver, 0)


def worker_fields(land, slots, offs, count):
    cx, ux, bd, g = (jnp.asarray(t) for t in tables())
    smem = pl.BlockSpec(memory_space=pltpu.SMEM)
    vmem = pl.BlockSpec(memory_space=pltpu.VMEM)
    return pl.pallas_call(
        pair_kernel,
        out_shape=jax.ShapeDtypeStruct((8, 32, 2, 16, 128), bf16),
        in_specs=[smem] * 3 + [vmem] * 5,
        out_specs=vmem,
        scratch_shapes=[
            pltpu.VMEM((4, CH, N, W), bf16),
            pltpu.VMEM((44, 96, 128), f32),
            pltpu.VMEM((2 * CH, N, 128), f32),
            pltpu.VMEM((32 * PITCH, 128), f32),
            pltpu.VMEM((32 * PITCH, 128), f32),
            pltpu.VMEM((4, CH, N, W), f32),
        ],
        compiler_params=pltpu.CompilerParams(vmem_limit_bytes=28 << 20),
        name="pairs",
    )(slots, offs, count, land, cx, ux, bd, g)


MESH = pl.DeviceIdType.MESH
SUBS = 4


def gather_kernel(gy, gx, orb, lists, land, *rest):
    blocks = rest[:8]
    wide, send, zsend, zrecv, ssem, rsem = rest[8:]
    G = gy * gx * 2
    me = lax.axis_index("grid")
    p = lax.axis_index("pair")
    my_y, my_x, my_c = me // (2 * gx), (me // 2) % gx, me % 2
    right, left = (p + 1) % 8, (p + 7) % 8
    held = blocks
    norb = orb.shape[1]
    pitch = norb + 4
    rows = norb // SUBS
    batch = min(4, G)

    def peer(i):
        y = (my_y + i // (2 * gx)) % gy
        x = (my_x + (i // 2) % gx) % gx
        c = (my_c + i) % 2
        return (y * gx + x) * 2 + c

    barrier = pltpu.get_barrier_semaphore()
    pl.semaphore_signal(barrier, inc=1, device_id=(me, right), device_id_type=MESH)
    pl.semaphore_signal(barrier, inc=1, device_id=(me, left), device_id_type=MESH)

    def greet(i, c):
        pl.semaphore_signal(barrier, inc=1, device_id=(peer(i), p), device_id_type=MESH)
        return c

    lax.fori_loop(1, G, greet, 0)

    def hop(d, h, sub):
        src, dst = (h - 1, h) if d == 0 else ((9 - h) % 8, 8 - h)
        part = pl.ds(sub * rows, rows)
        return pltpu.make_async_remote_copy(
            src_ref=held[src].at[part], dst_ref=held[dst].at[part],
            send_sem=zsend.at[d, h - 1, sub], recv_sem=zrecv.at[d, h - 1, sub],
            device_id=(me, left if d == 0 else right), device_id_type=MESH)

    def used(d, h, sub):
        return h < 4 or (h == 4 and (sub < SUBS // 2) == (d == 0))

    def pick(k):
        block = held[k]

        def some(t, c):
            for i in range(batch):
                g = t * batch + i
                for s in range(4):
                    send[k, g, s] = block[lists[p, s, g]]
            return c

        lax.fori_loop(0, G // batch, some, 0)

    def push(k):
        def one(i, c):
            g = peer(i)
            pltpu.make_async_remote_copy(
                src_ref=send.at[k, g], dst_ref=land.at[k, me], send_sem=ssem.at[k], recv_sem=rsem.at[k],
                device_id=(g, p), device_id_type=MESH).start()
            return c

        pltpu.make_async_copy(send.at[k, me], land.at[k, me], rsem.at[k]).start()
        lax.fori_loop(1, G, one, 0)

    for jj in range(2):
        for half in range(2):
            for xx in range(2):
                r = 4 * jj + 2 * half + xx
                lane = jj * 256 + half * 128
                wide[r * pitch:r * pitch + norb, :] = orb[xx, :, lane:lane + 128].astype(f32)

    def regroup(t, c):
        for i in range(8):
            o = t * 8 + i
            held[0][o] = wide[pl.ds(o, 8, stride=pitch), :].astype(bf16)
        return c

    lax.fori_loop(0, norb // 8, regroup, 0)
    pick(0)
    pl.semaphore_wait(barrier, G + 1)
    for sub in range(SUBS):
        for d in range(2):
            hop(d, 1, sub).start()
    push(0)
    for h in range(1, 5):
        for sub in range(SUBS):
            for d in range(2):
                if used(d, h, sub):
                    hop(d, h, sub).wait_recv()
                    if used(d, h + 1, sub):
                        hop(d, h + 1, sub).start()
        for k in (h, 8 - h) if h < 4 else (h,):
            pick(k)
            push(k)
    for h in range(1, 5):
        for sub in range(SUBS):
            for d in range(2):
                if used(d, h, sub):
                    hop(d, h, sub).wait_send()
    for k in range(8):
        pltpu.make_async_remote_copy(
            src_ref=send.at[k, pl.ds(1, G - 1)], dst_ref=land.at[k, pl.ds(1, G - 1)],
            send_sem=ssem.at[k], recv_sem=rsem.at[k], device_id=(me, right), device_id_type=MESH).wait_send()
        pltpu.make_async_copy(land.at[k], land.at[k], rsem.at[k]).wait()


def gather_boxes(orb, lists, gy, gx):
    G = gy * gx * 2
    norb = orb.shape[1]
    vmem = pl.BlockSpec(memory_space=pltpu.VMEM)
    return pl.pallas_call(
        lambda *refs: gather_kernel(gy, gx, *refs),
        out_shape=jax.ShapeDtypeStruct((8, G, 4, 8, 128), bf16),
        in_specs=[vmem, pl.BlockSpec(memory_space=pltpu.SMEM)],
        out_specs=vmem,
        scratch_shapes=[pltpu.VMEM((norb, 8, 128), bf16)] * 8 + [
            pltpu.VMEM((8 * (norb + 4), 128), f32),
            pltpu.VMEM((8, G, 4, 8, 128), bf16),
            pltpu.SemaphoreType.DMA((2, 4, SUBS)),
            pltpu.SemaphoreType.DMA((2, 4, SUBS)),
            pltpu.SemaphoreType.DMA((8,)),
            pltpu.SemaphoreType.DMA((8,)),
        ],
        compiler_params=pltpu.CompilerParams(collective_id=0, has_side_effects=True, vmem_limit_bytes=12 << 20),
        name="gather_boxes",
    )(orb, lists)


ORDER = ((4, None), (3, None), (5, None), (2, None), (6, None), (1, None), (7, None), (0, None))
NF, NS = 3, 5


def collect_kernel(gy, gx, norb, fields, lists, out, keys, rows, bufa, bufb, bufc, bufd, sumc, sumd, hot, hotc,
                   ssem, rsem, zsend, zrecv):
    G = gy * gx * 2
    HG = G // 2
    K = G * 16
    R = 4 * norb
    me = lax.axis_index("grid")
    p = lax.axis_index("pair")
    my_y, my_x, my_c = me // (2 * gx), (me // 2) % gx, me % 2
    toward = ((p + 1) % 8, (p + 7) % 8)

    def peer(i):
        y = (my_y + i // (2 * gx)) % gy
        x = (my_x + (i // 2) % gx) % gx
        c = (my_c + i) % 2
        return (y * gx + x) * 2 + c

    barrier = pltpu.get_barrier_semaphore()
    for z in toward:
        pl.semaphore_signal(barrier, inc=1, device_id=(me, z), device_id_type=MESH)

    def greet(i, c):
        pl.semaphore_signal(barrier, inc=1, device_id=(peer(i), p), device_id_type=MESH)
        return c

    lax.fori_loop(1, G, greet, 0)

    col_g = lax.broadcasted_iota(jnp.int32, (G, K), 1)
    row_g = lax.broadcasted_iota(jnp.int32, (G, K), 0)
    all_keys = ((lax.broadcasted_iota(jnp.int32, (8, K), 1) % 4) * norb).astype(f32)
    for s in range(4):
        pattern = (col_g // 16 == row_g) & (col_g // 4 % 4 == s)
        pattern = jnp.where(pattern, jnp.float32(1), jnp.float32(0)).astype(bf16)
        all_keys = all_keys + mm(lists[:, s, :].astype(f32).astype(bf16), pattern)
    keys[...] = all_keys.astype(jnp.int32)

    def choose(q, lo, n):
        key = keys[pl.ds(q, 1), lo:lo + n]
        rowid = lax.broadcasted_iota(jnp.int32, (R, n), 0)
        return jnp.where(rowid == key, jnp.float32(1), jnp.float32(0)).astype(bf16)

    hot[...] = choose(p, 0, K)
    pl.semaphore_wait(barrier, G + 1)

    def view(ref, k, g, h):
        return ref.at[k, g] if h is None else ref.at[k, g, h]

    def slot(k, h):
        return k

    def spread(k, h=None):
        sem = slot(k, h)
        pltpu.make_async_copy(view(fields, k, me, h), view(rows, k, me, h), rsem.at[sem]).start()

        def push(i, c):
            g = peer(i)
            pltpu.make_async_remote_copy(
                src_ref=view(fields, k, g, h), dst_ref=view(rows, k, me, h), send_sem=ssem.at[sem],
                recv_sem=rsem.at[sem], device_id=(g, p), device_id_type=MESH).start()
            return c

        lax.fori_loop(1, G, push, 0)

    def landed(k, h=None):
        part = view(rows, k, slice(None), h)
        pltpu.make_async_copy(part, part, rsem.at[slot(k, h)]).wait()

    def hop(d, stage, h):
        if stage == 0:
            src, dst = rows.at[4, pl.ds(d * HG, HG), h], bufa.at[d, h]
        elif stage == 1:
            src, dst = rows.at[(3, 5)[d], :, h], bufb.at[d, h, pl.ds(0, G)]
        elif stage == 2:
            src, dst = bufa.at[d, h], bufb.at[d, h, pl.ds(G, HG)]
        elif stage == 3:
            src, dst = sumc.at[d, h], bufc.at[d, h]
        else:
            src, dst = sumd.at[d, h], bufd.at[d, h]
        return pltpu.make_async_remote_copy(
            src_ref=src, dst_ref=dst, send_sem=zsend.at[d, stage, h], recv_sem=zrecv.at[d, stage, h],
            device_id=(me, toward[d]), device_id_type=MESH)

    def own(k, h):
        return mm(hot[...], rows[k, :, h].reshape(K, 128))

    for k, h in ORDER[:NF]:
        spread(k, h)
    landed(4)
    for h in range(2):
        for d in range(2):
            hop(d, 0, h).start()
    for k, h in ORDER[NF:NS]:
        spread(k, h)
    for d in range(2):
        q1, q2 = ((p + 7) % 8, (p + 6) % 8) if d == 0 else ((p + 1) % 8, (p + 2) % 8)
        hotc[d, :, 0:K] = choose(q1, 0, K)
        hotc[d, :, K:K + K // 2] = choose(q2, d * (K // 2), K // 2)
    for h in range(2):
        for d in range(2):
            if h == 0:
                landed((3, 5)[d])
            hop(d, 1, h).start()
            hop(d, 0, h).wait_recv()
            hop(d, 2, h).start()
    for k, h in ORDER[NS:]:
        spread(k, h)
    landed(2)
    landed(6)
    for h in range(2):
        for d in range(2):
            hop(d, 1, h).wait_recv()
            hop(d, 2, h).wait_recv()
            sumc[d, h] = own((2, 6)[d], h) + mm(hotc[d], bufb[d, h].reshape(K + K // 2, 128))
            hop(d, 3, h).start()
    landed(1)
    landed(7)
    landed(0)
    mine = [own(0, h) for h in range(2)]
    for h in range(2):
        for d in range(2):
            part = own((1, 7)[d], h)
            hop(d, 3, h).wait_recv()
            sumd[d, h] = (part + bufc[d, h]).astype(bf16)
            hop(d, 4, h).start()
    for h in range(2):
        for d in range(2):
            hop(d, 4, h).wait_recv()
        total = mine[h] + bufd[0, h].astype(f32) + bufd[1, h].astype(f32)
        for jj in range(2):
            for xx in range(2):
                i = jj * 2 + xx
                out[xx, :, jj * 256 + h * 128:jj * 256 + (h + 1) * 128] = total[i * norb:(i + 1) * norb]
    for d in range(2):
        for stage in range(5):
            for h in range(2):
                hop(d, stage, h).wait_send()
    for k, h in ORDER:
        many = pl.ds(1, G - 1)
        pltpu.make_async_remote_copy(
            src_ref=view(fields, k, many, h), dst_ref=view(rows, k, many, h), send_sem=ssem.at[slot(k, h)],
            recv_sem=rsem.at[slot(k, h)], device_id=(me, toward[0]), device_id_type=MESH).wait_send()


def collect_fields(fields, lists, norb, gy, gx):
    G = gy * gx * 2
    vmem = pl.BlockSpec(memory_space=pltpu.VMEM)
    sums = pltpu.VMEM((2, 2, 4 * norb, 128), f32)
    last = pltpu.VMEM((2, 2, 4 * norb, 128), bf16)
    return pl.pallas_call(
        lambda *refs: collect_kernel(gy, gx, norb, *refs),
        out_shape=jax.ShapeDtypeStruct((2, norb, 512), f32),
        in_specs=[vmem, vmem],
        out_specs=vmem,
        scratch_shapes=[
            pltpu.VMEM((8, G * 16), jnp.int32),
            pltpu.VMEM((8, G, 2, 16, 128), bf16),
            pltpu.VMEM((2, 2, G // 2, 16, 128), bf16),
            pltpu.VMEM((2, 2, G + G // 2, 16, 128), bf16),
            sums, last, sums, last,
            pltpu.VMEM((4 * norb, G * 16), bf16),
            pltpu.VMEM((2, 4 * norb, G * 24), bf16),
            pltpu.SemaphoreType.DMA((10,)),
            pltpu.SemaphoreType.DMA((10,)),
            pltpu.SemaphoreType.DMA((2, 5, 2)),
            pltpu.SemaphoreType.DMA((2, 5, 2)),
        ],
        compiler_params=pltpu.CompilerParams(collective_id=1, has_side_effects=True, vmem_limit_bytes=18 << 20),
        name="collect_fields",
    )(fields, lists)


def shards(orbitals, box_list, pair_slots, offsets, pair_count):
    lists = jnp.transpose(box_list, (1, 2, 0))
    slots = jnp.transpose(pair_slots, (0, 1, 3, 2)).reshape(2, 4)
    offs = jnp.transpose(offsets, (0, 3, 1, 2)).reshape(3, 1, 4)
    land = gather_boxes(orbitals, lists, 4, 4)
    fields = worker_fields(land, slots, offs, pair_count)
    return collect_fields(fields, lists, orbitals.shape[1], 4, 4)


def solution(mesh):
    placed = (
        P("grid", None, "pair"),
        P(),
        P("grid", "pair", None, None),
        P("grid", "pair", None, None),
        P("grid", "pair"),
    )
    return jax.shard_map(
        shards, mesh=mesh, in_specs=placed, out_specs=P("grid", None, "pair"), check_vma=False
    )
```

```python
import math
import numpy as np
import jax
import jax.numpy as jnp
from jax import lax
from jax.experimental import pallas as pl
from jax.experimental.pallas import tpu as pltpu
from jax.sharding import PartitionSpec as P

screening = 0.02
N = 64
CH = 16
W = 256
PITCH = 68
PITCH2 = 20
PITCH3 = 36
f32, bf16 = jnp.float32, jnp.bfloat16


def tables():
    m = np.arange(N)
    ph = 2.0 * math.pi * ((m[:, None] * m[None, :]) % N) / N
    cas = np.cos(ph) + np.sin(ph)
    perm = np.concatenate([np.arange(0, N, 2), np.arange(1, N, 2)])

    def parts(a):
        a = np.asarray(a, np.float32)
        hi = a.astype(bf16)
        lo = (a - hi.astype(np.float32)).astype(bf16)
        return hi, lo

    def left(a):
        hi, lo = parts(a)
        return np.concatenate([hi, hi, lo], axis=1)

    cx = left(cas[:, perm])
    ux = left(cas[perm, :])
    cf = left(cas[:, perm])
    ci = left(cas[perm, :])
    hi, lo = parts(np.kron(np.eye(4), cas))
    bd = np.concatenate([hi, hi, lo], axis=0)
    e = 2.0 - 2.0 * np.cos(2.0 * math.pi * m / N)
    green = 1.0 / ((screening + e[:, None, None] + e[None, :, None] + e[None, None, :]) * float(N**3))
    g = green.reshape(CH, 4, N, N).transpose(0, 2, 1, 3).reshape(CH, N, W).astype(np.float32)
    return cx, ux, bd, g


def split(v):
    hi = v.astype(bf16)
    lo = (v - hi.astype(f32)).astype(bf16)
    return hi, lo


def mm(a, b):
    return jnp.dot(a, b, preferred_element_type=f32)


def left_mul(table, v):
    hi, lo = split(v)
    return mm(table, jnp.concatenate([hi, lo, hi], axis=0))


def right_mul(v, bd):
    hi, lo = split(v)
    return mm(jnp.concatenate([hi, lo, hi], axis=1), bd)


def pair_kernel(slots, offs, count, box, cx, ux, bd, green, col, S, SH, U):
    low = lax.broadcasted_iota(jnp.int32, (32, 128), 1) < 64
    lane = lax.broadcasted_iota(jnp.int32, (N, 128), 1)
    for r in (slice(0, 6), slice(38, 44)):
        S[r] = jnp.zeros((6, 96, 128), f32)
    for r in (0, 40, 48, 88):
        S[6:38, r:r + 8, :] = jnp.zeros((32, 8, 128), f32)
    col[...] = jnp.zeros(col.shape, f32)

    def pair(k, carry):
        a = slots[0, k]
        b = slots[1, k]
        dx, dy, dz = offs[0, 0, k], offs[1, 0, k], offs[2, 0, k]
        t = dy * 64 + dz
        q = (t + 1024) // 128 - 8
        r = t - 128 * q
        z = lane % 64
        inside = (z + dz >= 0) & (z + dz < 64)
        inside_back = (z - dz >= 0) & (z - dz < 64)

        def put(j, v):
            for h in range(2):
                for e in range(2):
                    S[6 + 2 * j + h, e * 48 + 8:e * 48 + 40, :] = v[e * 32:(e + 1) * 32, h * 128:(h + 1) * 128]

        def fetch(tile, step, turn):
            both = []
            for e in range(2):
                n = step + 16 + e
                both.append(S[tile, pl.ds(n % 2 * 48 + n // 2, 32), :])
            return pltpu.roll(jnp.concatenate(both, axis=0), turn, 1)

        for j in range(CH):
            put(j, box[b, j].astype(f32))
        turn = (128 - r) % 128
        here = fetch(6 + q, dx, turn)
        for T in range(2 * CH):
            then = fetch(7 + T + q, dx, turn)
            SH[T] = jnp.where(inside, jnp.where(lane < 128 - r, here, then), jnp.float32(0))
            here = then

        outs = []
        for j in range(CH):
            moved = jnp.concatenate([SH[2 * j], SH[2 * j + 1]], axis=1)
            outs.append(left_mul(cx[...], box[a, j].astype(f32) * moved))
        spec = right_mul(jnp.concatenate(outs, axis=0), bd[...])
        for j in range(CH):
            for h in range(2):
                U[(2 * j + h) * PITCH:(2 * j + h) * PITCH + N, :] = spec[j * N:(j + 1) * N, h * 128:(h + 1) * 128]

        def middle(g, c):
            tops, bots = [], []
            for h in range(2):
                l1 = U[pl.ds(g * 4 + 2 * h, 32, stride=PITCH), :]
                l2 = U[pl.ds(g * 4 + 2 * h + 1, 32, stride=PITCH), :]
                tops.append(jnp.where(low, l1, pltpu.roll(l2, 64, 1)))
                bots.append(jnp.where(low, pltpu.roll(l1, 64, 1), l2))
            v = jnp.concatenate([jnp.concatenate(tops, axis=1), jnp.concatenate(bots, axis=1)], axis=0)
            s = left_mul(cx[...], v) * green[g]
            p = left_mul(ux[...], s)
            for h in range(2):
                x0 = p[:32, h * 128:(h + 1) * 128]
                x1 = p[32:, h * 128:(h + 1) * 128]
                U[pl.ds(g * 4 + 2 * h, 32, stride=PITCH), :] = jnp.where(low, x0, pltpu.roll(x1, 64, 1))
                U[pl.ds(g * 4 + 2 * h + 1, 32, stride=PITCH), :] = jnp.where(low, pltpu.roll(x0, 64, 1), x1)
            return c

        lax.fori_loop(0, CH, middle, 0, unroll=8)

        outs = []
        for j in range(CH):
            v = jnp.concatenate([U[(2 * j + h) * PITCH:(2 * j + h) * PITCH + N, :] for h in range(2)], axis=1)
            outs.append(left_mul(ux[...], v))
        pot = right_mul(jnp.concatenate(outs, axis=0), bd[...]).reshape(CH, N, W)
        for j in range(CH):
            moved = jnp.concatenate([SH[2 * j], SH[2 * j + 1]], axis=1)
            col[a, j] = col[a, j] - pot[j] * moved
            put(j, -(pot[j] * box[a, j].astype(f32)))

        here = fetch(5 - q, -dx, r)
        for T in range(2 * CH):
            then = fetch(6 + T - q, -dx, r)
            u = jnp.where(inside_back, jnp.where(lane < r, here, then), jnp.float32(0))
            part = slice(T % 2 * 128, T % 2 * 128 + 128)
            col[b, T // 2, :, part] = col[b, T // 2, :, part] + u
            here = then
        return carry

    lax.fori_loop(0, count[0, 0], pair, 0)


def worker_fields(box, slots, offs, count):
    cx, ux, bd, g = (jnp.asarray(t) for t in tables())
    smem = pl.BlockSpec(memory_space=pltpu.SMEM)
    vmem = pl.BlockSpec(memory_space=pltpu.VMEM)
    return pl.pallas_call(
        pair_kernel,
        out_shape=jax.ShapeDtypeStruct((4, CH, N, W), f32),
        in_specs=[smem] * 3 + [vmem] * 5,
        out_specs=vmem,
        scratch_shapes=[
            pltpu.VMEM((44, 96, 128), f32),
            pltpu.VMEM((2 * CH, N, 128), f32),
            pltpu.VMEM((33 * PITCH, 128), f32),
        ],
        compiler_params=pltpu.CompilerParams(vmem_limit_bytes=28 << 20),
        name="pairs",
    )(slots, offs, count, box, cx, ux, bd, g)


MESH = pl.DeviceIdType.MESH
SUBS = 4


def gather_kernel(gy, gx, orb, lists, box, *rest):
    blocks = rest[:8]
    wide, F, land, send, zsend, zrecv, ssem, rsem = rest[8:]
    G = gy * gx * 2
    me = lax.axis_index("grid")
    p = lax.axis_index("pair")
    my_y, my_x, my_c = me // (2 * gx), (me // 2) % gx, me % 2
    right, left = (p + 1) % 8, (p + 7) % 8
    held = blocks
    norb = orb.shape[1]
    pitch = norb + 4
    rows = norb // SUBS
    batch = min(4, G)

    across = [((my_x + i // 2) % gx) * 2 + (my_c + i) % 2 for i in range(2 * gx)]

    def each_peer(act):
        for i in range(1, 2 * gx):
            act(my_y * (2 * gx) + across[i])

        def line(i, c):
            y = (my_y + i) % gy * (2 * gx)
            for a in across:
                act(y + a)
            return c

        lax.fori_loop(1, gy, line, 0)

    barrier = pltpu.get_barrier_semaphore()
    pl.semaphore_signal(barrier, inc=1, device_id=(me, right), device_id_type=MESH)
    pl.semaphore_signal(barrier, inc=1, device_id=(me, left), device_id_type=MESH)

    each_peer(lambda g: pl.semaphore_signal(barrier, inc=1, device_id=(g, p), device_id_type=MESH))

    def hop(d, h, sub):
        src, dst = (h - 1, h) if d == 0 else ((9 - h) % 8, 8 - h)
        part = pl.ds(sub * rows, rows)
        return pltpu.make_async_remote_copy(
            src_ref=held[src].at[part], dst_ref=held[dst].at[part],
            send_sem=zsend.at[d, h - 1, sub], recv_sem=zrecv.at[d, h - 1, sub],
            device_id=(me, left if d == 0 else right), device_id_type=MESH)

    def used(d, h, sub):
        return h < 4 or (h == 4 and (sub < SUBS // 2) == (d == 0))

    def pick(k):
        block = held[k]

        def some(t, c):
            for i in range(batch):
                g = t * batch + i
                for s in range(4):
                    send[k, g, s] = block[lists[p, s, g]]
            return c

        lax.fori_loop(0, G // batch, some, 0)

    def push(k):
        def one(g):
            pltpu.make_async_remote_copy(
                src_ref=send.at[k, g], dst_ref=land.at[k, me], send_sem=ssem.at[k], recv_sem=rsem.at[k],
                device_id=(g, p), device_id_type=MESH).start()

        pltpu.make_async_copy(send.at[k, me], land.at[k, me], rsem.at[k]).start()
        each_peer(one)

    for jj in range(2):
        for half in range(2):
            for xx in range(2):
                r = 4 * jj + 2 * half + xx
                lane = jj * 256 + half * 128
                wide[r * pitch:r * pitch + norb, :] = orb[xx, :, lane:lane + 128].astype(f32)

    def regroup(t, c):
        for i in range(8):
            o = t * 8 + i
            held[0][o] = wide[pl.ds(o, 8, stride=pitch), :].astype(bf16)
        return c

    lax.fori_loop(0, norb // 8, regroup, 0)
    pick(0)
    pl.semaphore_wait(barrier, G + 1)
    for sub in range(SUBS):
        for d in range(2):
            hop(d, 1, sub).start()
    push(0)
    for h in range(1, 5):
        for sub in range(SUBS):
            for d in range(2):
                if used(d, h, sub):
                    hop(d, h, sub).wait_recv()
                    if used(d, h + 1, sub):
                        hop(d, h + 1, sub).start()
        for k in (h, 8 - h) if h < 4 else (h,):
            pick(k)
            push(k)

    for k in (0, 1, 7, 2, 6, 3, 5, 4):
        pltpu.make_async_copy(land.at[k], land.at[k], rsem.at[k]).wait()

        def widen(t, c):
            for i in range(batch):
                g = t * batch + i
                for s in range(4):
                    F[pl.ds(pl.multiple_of(g * PITCH3, 4) + 8 * s, 8), :] = land[k, g, s].astype(f32)
            return c

        lax.fori_loop(0, G // batch, widen, 0)
        j = (p + k) % 8 * 2
        for s in range(4):
            for jj in range(2):
                for half in range(2):
                    for xx in range(2):
                        part = F[pl.ds(8 * s + 4 * jj + 2 * half + xx, G, stride=PITCH3), :]
                        box[s, j + jj, xx * G:(xx + 1) * G, half * 128:(half + 1) * 128] = part.astype(bf16)
    for h in range(1, 5):
        for sub in range(SUBS):
            for d in range(2):
                if used(d, h, sub):
                    hop(d, h, sub).wait_send()
    for k in range(8):
        pltpu.make_async_remote_copy(
            src_ref=send.at[k, pl.ds(1, G - 1)], dst_ref=land.at[k, pl.ds(1, G - 1)],
            send_sem=ssem.at[k], recv_sem=rsem.at[k], device_id=(me, right), device_id_type=MESH).wait_send()


def gather_boxes(orb, lists, gy, gx):
    G = gy * gx * 2
    norb = orb.shape[1]
    vmem = pl.BlockSpec(memory_space=pltpu.VMEM)
    return pl.pallas_call(
        lambda *refs: gather_kernel(gy, gx, *refs),
        out_shape=jax.ShapeDtypeStruct((4, 16, 2 * G, 256), bf16),
        in_specs=[vmem, pl.BlockSpec(memory_space=pltpu.SMEM)],
        out_specs=vmem,
        scratch_shapes=[pltpu.VMEM((norb, 8, 128), bf16)] * 8 + [
            pltpu.VMEM((9 * (norb + 4), 128), f32),
            pltpu.VMEM(((G + 1) * PITCH3, 128), f32),
            pltpu.VMEM((8, G, 4, 8, 128), bf16),
            pltpu.VMEM((8, G, 4, 8, 128), bf16),
            pltpu.SemaphoreType.DMA((2, 4, SUBS)),
            pltpu.SemaphoreType.DMA((2, 4, SUBS)),
            pltpu.SemaphoreType.DMA((8,)),
            pltpu.SemaphoreType.DMA((8,)),
        ],
        compiler_params=pltpu.CompilerParams(collective_id=0, has_side_effects=True, vmem_limit_bytes=16 << 20),
        name="gather_boxes",
    )(orb, lists)


ORDER = ((4, None), (3, None), (5, None), (2, None), (6, None), (1, None), (7, None), (0, None))
NF, NS = 3, 5


def collect_kernel(gy, gx, norb, col, lists, out, F, fields, keys, rows, bufa, bufb, bufc, bufd, sumc, sumd, hot, hotc,
                   ssem, rsem, zsend, zrecv):
    G = gy * gx * 2
    HG = G // 2
    K = G * 16
    R = 4 * norb
    me = lax.axis_index("grid")
    p = lax.axis_index("pair")
    my_y, my_x, my_c = me // (2 * gx), (me // 2) % gx, me % 2
    toward = ((p + 1) % 8, (p + 7) % 8)

    across = [((my_x + i // 2) % gx) * 2 + (my_c + i) % 2 for i in range(2 * gx)]

    def each_peer(act):
        for i in range(1, 2 * gx):
            act(my_y * (2 * gx) + across[i])

        def line(i, c):
            y = (my_y + i) % gy * (2 * gx)
            for a in across:
                act(y + a)
            return c

        lax.fori_loop(1, gy, line, 0)

    barrier = pltpu.get_barrier_semaphore()
    for z in toward:
        pl.semaphore_signal(barrier, inc=1, device_id=(me, z), device_id_type=MESH)

    each_peer(lambda g: pl.semaphore_signal(barrier, inc=1, device_id=(g, p), device_id_type=MESH))

    def choose(q, lo, n):
        key = keys[pl.ds(q, 1), lo:lo + n]
        rowid = lax.broadcasted_iota(jnp.int32, (R, n), 0)
        return jnp.where(rowid == key, jnp.float32(1), jnp.float32(0)).astype(bf16)

    batch = min(4, G)

    def deliver(k):
        j = (p + k) % 8 * 2
        for s in range(4):
            for jj in range(2):
                for half in range(2):
                    for xx in range(2):
                        F[pl.ds(G * PITCH2 * half + 4 * s + 2 * jj + xx, G, stride=PITCH2), :] = (
                            col[s, j + jj, xx * G:(xx + 1) * G, half * 128:(half + 1) * 128])

        def narrow(t, c):
            for i in range(batch):
                g = t * batch + i
                for half in range(2):
                    fields[k, g, half] = F[pl.ds(pl.multiple_of((half * G + g) * PITCH2, 4), 16), :].astype(bf16)
            return c

        lax.fori_loop(0, G // batch, narrow, 0)

    deliver(ORDER[0][0])
    pl.semaphore_wait(barrier, G + 1)

    def view(ref, k, g, h):
        return ref.at[k, g] if h is None else ref.at[k, g, h]

    def slot(k, h):
        return k

    def spread(k, h=None):
        sem = slot(k, h)
        pltpu.make_async_copy(view(fields, k, me, h), view(rows, k, me, h), rsem.at[sem]).start()

        def push(g):
            pltpu.make_async_remote_copy(
                src_ref=view(fields, k, g, h), dst_ref=view(rows, k, me, h), send_sem=ssem.at[sem],
                recv_sem=rsem.at[sem], device_id=(g, p), device_id_type=MESH).start()

        each_peer(push)

    def landed(k, h=None):
        part = view(rows, k, slice(None), h)
        pltpu.make_async_copy(part, part, rsem.at[slot(k, h)]).wait()

    def hop(d, stage, h):
        if stage == 0:
            src, dst = rows.at[4, pl.ds(d * HG, HG), h], bufa.at[d, h]
        elif stage == 1:
            src, dst = rows.at[(3, 5)[d], :, h], bufb.at[d, h, pl.ds(0, G)]
        elif stage == 2:
            src, dst = bufa.at[d, h], bufb.at[d, h, pl.ds(G, HG)]
        elif stage == 3:
            src, dst = sumc.at[d, h], bufc.at[d, h]
        else:
            src, dst = sumd.at[d, h], bufd.at[d, h]
        return pltpu.make_async_remote_copy(
            src_ref=src, dst_ref=dst, send_sem=zsend.at[d, stage, h], recv_sem=zrecv.at[d, stage, h],
            device_id=(me, toward[d]), device_id_type=MESH)

    def own(k, h):
        return mm(hot[...], rows[k, :, h].reshape(K, 128))

    def spread_many(lo, hi):
        for n in range(lo, hi):
            if n + 1 < len(ORDER):
                deliver(ORDER[n + 1][0])
            spread(*ORDER[n])

    spread_many(0, NF)
    col_g = lax.broadcasted_iota(jnp.int32, (G, K), 1)
    row_g = lax.broadcasted_iota(jnp.int32, (G, K), 0)
    all_keys = ((lax.broadcasted_iota(jnp.int32, (8, K), 1) % 4) * norb).astype(f32)
    for s in range(4):
        pattern = (col_g // 16 == row_g) & (col_g // 4 % 4 == s)
        pattern = jnp.where(pattern, jnp.float32(1), jnp.float32(0)).astype(bf16)
        all_keys = all_keys + mm(lists[:, s, :].astype(f32).astype(bf16), pattern)
    keys[...] = all_keys.astype(jnp.int32)

    hot[...] = choose(p, 0, K)
    landed(4)
    for h in range(2):
        for d in range(2):
            hop(d, 0, h).start()
    spread_many(NF, NS)
    for d in range(2):
        q1, q2 = ((p + 7) % 8, (p + 6) % 8) if d == 0 else ((p + 1) % 8, (p + 2) % 8)
        hotc[d, :, 0:K] = choose(q1, 0, K)
        hotc[d, :, K:K + K // 2] = choose(q2, d * (K // 2), K // 2)
    for h in range(2):
        for d in range(2):
            if h == 0:
                landed((3, 5)[d])
            hop(d, 1, h).start()
            hop(d, 0, h).wait_recv()
            hop(d, 2, h).start()
    spread_many(NS, len(ORDER))
    landed(2)
    landed(6)
    for h in range(2):
        for d in range(2):
            hop(d, 1, h).wait_recv()
            hop(d, 2, h).wait_recv()
            sumc[d, h] = own((2, 6)[d], h) + mm(hotc[d], bufb[d, h].reshape(K + K // 2, 128))
            hop(d, 3, h).start()
    landed(1)
    landed(7)
    landed(0)
    mine = [own(0, h) for h in range(2)]
    for h in range(2):
        for d in range(2):
            part = own((1, 7)[d], h)
            hop(d, 3, h).wait_recv()
            sumd[d, h] = (part + bufc[d, h]).astype(bf16)
            hop(d, 4, h).start()
    for h in range(2):
        for d in range(2):
            hop(d, 4, h).wait_recv()
        total = mine[h] + bufd[0, h].astype(f32) + bufd[1, h].astype(f32)
        for jj in range(2):
            for xx in range(2):
                i = jj * 2 + xx
                out[xx, :, jj * 256 + h * 128:jj * 256 + (h + 1) * 128] = total[i * norb:(i + 1) * norb]
    for d in range(2):
        for stage in range(5):
            for h in range(2):
                hop(d, stage, h).wait_send()
    for k, h in ORDER:
        many = pl.ds(1, G - 1)
        pltpu.make_async_remote_copy(
            src_ref=view(fields, k, many, h), dst_ref=view(rows, k, many, h), send_sem=ssem.at[slot(k, h)],
            recv_sem=rsem.at[slot(k, h)], device_id=(me, toward[0]), device_id_type=MESH).wait_send()


def collect_fields(col, lists, norb, gy, gx):
    G = gy * gx * 2
    vmem = pl.BlockSpec(memory_space=pltpu.VMEM)
    sums = pltpu.VMEM((2, 2, 4 * norb, 128), f32)
    last = pltpu.VMEM((2, 2, 4 * norb, 128), bf16)
    return pl.pallas_call(
        lambda *refs: collect_kernel(gy, gx, norb, *refs),
        out_shape=jax.ShapeDtypeStruct((2, norb, 512), f32),
        in_specs=[vmem, vmem],
        out_specs=vmem,
        scratch_shapes=[
            pltpu.VMEM(((2 * G + 1) * PITCH2, 128), f32),
            pltpu.VMEM((8, G, 2, 16, 128), bf16),
            pltpu.VMEM((8, G * 16), jnp.int32),
            pltpu.VMEM((8, G, 2, 16, 128), bf16),
            pltpu.VMEM((2, 2, G // 2, 16, 128), bf16),
            pltpu.VMEM((2, 2, G + G // 2, 16, 128), bf16),
            sums, last, sums, last,
            pltpu.VMEM((4 * norb, G * 16), bf16),
            pltpu.VMEM((2, 4 * norb, G * 24), bf16),
            pltpu.SemaphoreType.DMA((10,)),
            pltpu.SemaphoreType.DMA((10,)),
            pltpu.SemaphoreType.DMA((2, 5, 2)),
            pltpu.SemaphoreType.DMA((2, 5, 2)),
        ],
        compiler_params=pltpu.CompilerParams(collective_id=1, has_side_effects=True, vmem_limit_bytes=22 << 20),
        name="collect_fields",
    )(col, lists)


def shards(orbitals, box_list, pair_slots, offsets, pair_count):
    lists = jnp.transpose(box_list, (1, 2, 0))
    slots = jnp.transpose(pair_slots, (0, 1, 3, 2)).reshape(2, 4)
    offs = jnp.transpose(offsets, (0, 3, 1, 2)).reshape(3, 1, 4)
    box = gather_boxes(orbitals, lists, 4, 4)
    col = worker_fields(box, slots, offs, pair_count)
    return collect_fields(col, lists, orbitals.shape[1], 4, 4)


def solution(mesh):
    placed = (
        P("grid", None, "pair"),
        P(),
        P("grid", "pair", None, None),
        P("grid", "pair", None, None),
        P("grid", "pair"),
    )
    return jax.shard_map(
        shards, mesh=mesh, in_specs=placed, out_specs=P("grid", None, "pair"), check_vma=False
    )
```

```python
import math
import numpy as np
import jax
import jax.numpy as jnp
from jax import lax
from jax.experimental import pallas as pl
from jax.experimental.pallas import tpu as pltpu
from jax.sharding import PartitionSpec as P

screening = 0.02
N = 64
CH = 16
W = 256
PITCH = 68
PITCH2 = 20
PITCH3 = 36
f32, bf16 = jnp.float32, jnp.bfloat16


def tables():
    m = np.arange(N)
    ph = 2.0 * math.pi * ((m[:, None] * m[None, :]) % N) / N
    cas = np.cos(ph) + np.sin(ph)
    perm = np.concatenate([np.arange(0, N, 2), np.arange(1, N, 2)])

    def parts(a):
        a = np.asarray(a, np.float32)
        hi = a.astype(bf16)
        lo = (a - hi.astype(np.float32)).astype(bf16)
        return hi, lo

    def left(a):
        hi, lo = parts(a)
        return np.concatenate([hi, hi, lo], axis=1)

    cx = left(cas[:, perm])
    ux = left(cas[perm, :])
    cf = left(cas[:, perm])
    ci = left(cas[perm, :])
    hi, lo = parts(np.kron(np.eye(4), cas))
    bd = np.concatenate([hi, hi, lo], axis=0)
    e = 2.0 - 2.0 * np.cos(2.0 * math.pi * m / N)
    green = 1.0 / ((screening + e[:, None, None] + e[None, :, None] + e[None, None, :]) * float(N**3))
    g = green.reshape(CH, 4, N, N).transpose(0, 2, 1, 3).reshape(CH, N, W).astype(np.float32)
    return cx, ux, bd, g


def split(v):
    hi = v.astype(bf16)
    lo = (v - hi.astype(f32)).astype(bf16)
    return hi, lo


def mm(a, b):
    return jnp.dot(a, b, preferred_element_type=f32)


def left_mul(table, v):
    hi, lo = split(v)
    return mm(table, jnp.concatenate([hi, lo, hi], axis=0))


def right_mul(v, bd):
    hi, lo = split(v)
    return mm(jnp.concatenate([hi, lo, hi], axis=1), bd)


def pair_kernel(slots, offs, count, box, cx, ux, bd, green, col, S, SH, U):
    low = lax.broadcasted_iota(jnp.int32, (32, 128), 1) < 64
    lane = lax.broadcasted_iota(jnp.int32, (N, 128), 1)
    for r in (slice(0, 6), slice(38, 44)):
        S[r] = jnp.zeros((6, 96, 128), f32)
    for r in (0, 40, 48, 88):
        S[6:38, r:r + 8, :] = jnp.zeros((32, 8, 128), f32)
    col[...] = jnp.zeros(col.shape, f32)

    def pair(k, carry):
        a = slots[0, k]
        b = slots[1, k]
        dx, dy, dz = offs[0, 0, k], offs[1, 0, k], offs[2, 0, k]
        t = dy * 64 + dz
        q = (t + 1024) // 128 - 8
        r = t - 128 * q
        z = lane % 64
        inside = (z + dz >= 0) & (z + dz < 64)
        inside_back = (z - dz >= 0) & (z - dz < 64)

        def put(j, v):
            for h in range(2):
                for e in range(2):
                    S[6 + 2 * j + h, e * 48 + 8:e * 48 + 40, :] = v[e * 32:(e + 1) * 32, h * 128:(h + 1) * 128]

        def fetch(tile, step, turn):
            both = []
            for e in range(2):
                n = step + 16 + e
                both.append(S[tile, pl.ds(n % 2 * 48 + n // 2, 32), :])
            return pltpu.roll(jnp.concatenate(both, axis=0), turn, 1)

        for j in range(CH):
            put(j, box[b, j].astype(f32))
        turn = (128 - r) % 128
        here = fetch(6 + q, dx, turn)
        for T in range(2 * CH):
            then = fetch(7 + T + q, dx, turn)
            SH[T] = jnp.where(inside, jnp.where(lane < 128 - r, here, then), jnp.float32(0))
            here = then

        outs = []
        for j in range(CH):
            moved = jnp.concatenate([SH[2 * j], SH[2 * j + 1]], axis=1)
            outs.append(left_mul(cx[...], box[a, j].astype(f32) * moved))
        spec = right_mul(jnp.concatenate(outs, axis=0), bd[...])
        for j in range(CH):
            for h in range(2):
                U[(2 * j + h) * PITCH:(2 * j + h) * PITCH + N, :] = spec[j * N:(j + 1) * N, h * 128:(h + 1) * 128]

        def middle(g, c):
            tops, bots = [], []
            for h in range(2):
                l1 = U[pl.ds(g * 4 + 2 * h, 32, stride=PITCH), :]
                l2 = U[pl.ds(g * 4 + 2 * h + 1, 32, stride=PITCH), :]
                tops.append(jnp.where(low, l1, pltpu.roll(l2, 64, 1)))
                bots.append(jnp.where(low, pltpu.roll(l1, 64, 1), l2))
            v = jnp.concatenate([jnp.concatenate(tops, axis=1), jnp.concatenate(bots, axis=1)], axis=0)
            s = left_mul(cx[...], v) * green[g]
            p = left_mul(ux[...], s)
            for h in range(2):
                x0 = p[:32, h * 128:(h + 1) * 128]
                x1 = p[32:, h * 128:(h + 1) * 128]
                U[pl.ds(g * 4 + 2 * h, 32, stride=PITCH), :] = jnp.where(low, x0, pltpu.roll(x1, 64, 1))
                U[pl.ds(g * 4 + 2 * h + 1, 32, stride=PITCH), :] = jnp.where(low, pltpu.roll(x0, 64, 1), x1)
            return c

        lax.fori_loop(0, CH, middle, 0, unroll=8)

        outs = []
        for j in range(CH):
            v = jnp.concatenate([U[(2 * j + h) * PITCH:(2 * j + h) * PITCH + N, :] for h in range(2)], axis=1)
            outs.append(left_mul(ux[...], v))
        pot = right_mul(jnp.concatenate(outs, axis=0), bd[...]).reshape(CH, N, W)
        for j in range(CH):
            moved = jnp.concatenate([SH[2 * j], SH[2 * j + 1]], axis=1)
            col[a, j] = col[a, j] - pot[j] * moved
            put(j, -(pot[j] * box[a, j].astype(f32)))

        here = fetch(5 - q, -dx, r)
        for T in range(2 * CH):
            then = fetch(6 + T - q, -dx, r)
            u = jnp.where(inside_back, jnp.where(lane < r, here, then), jnp.float32(0))
            part = slice(T % 2 * 128, T % 2 * 128 + 128)
            col[b, T // 2, :, part] = col[b, T // 2, :, part] + u
            here = then
        return carry

    lax.fori_loop(0, count[0, 0], pair, 0)


def worker_fields(box, slots, offs, count):
    cx, ux, bd, g = (jnp.asarray(t) for t in tables())
    smem = pl.BlockSpec(memory_space=pltpu.SMEM)
    vmem = pl.BlockSpec(memory_space=pltpu.VMEM)
    return pl.pallas_call(
        pair_kernel,
        out_shape=jax.ShapeDtypeStruct((4, CH, N, W), f32),
        in_specs=[smem] * 3 + [vmem] * 5,
        out_specs=vmem,
        scratch_shapes=[
            pltpu.VMEM((44, 96, 128), f32),
            pltpu.VMEM((2 * CH, N, 128), f32),
            pltpu.VMEM((33 * PITCH, 128), f32),
        ],
        compiler_params=pltpu.CompilerParams(vmem_limit_bytes=28 << 20),
        name="pairs",
    )(slots, offs, count, box, cx, ux, bd, g)


MESH = pl.DeviceIdType.MESH
SUBS = 4


def gather_kernel(gy, gx, orb, lists, box, *rest):
    blocks = rest[:8]
    wide, F, land, send, zsend, zrecv, ssem, rsem = rest[8:]
    G = gy * gx * 2
    me = lax.axis_index("grid")
    p = lax.axis_index("pair")
    my_y, my_x, my_c = me // (2 * gx), (me // 2) % gx, me % 2
    right, left = (p + 1) % 8, (p + 7) % 8
    held = blocks
    norb = orb.shape[1]
    pitch = norb + 4
    rows = norb // SUBS
    batch = min(4, G)

    across = [((my_x + i // 2) % gx) * 2 + (my_c + i) % 2 for i in range(2 * gx)]

    def each_peer(act):
        for i in range(1, 2 * gx):
            act(my_y * (2 * gx) + across[i])

        def line(i, c):
            y = (my_y + i) % gy * (2 * gx)
            for a in across:
                act(y + a)
            return c

        lax.fori_loop(1, gy, line, 0)

    barrier = pltpu.get_barrier_semaphore()
    pl.semaphore_signal(barrier, inc=1, device_id=(me, right), device_id_type=MESH)
    pl.semaphore_signal(barrier, inc=1, device_id=(me, left), device_id_type=MESH)

    each_peer(lambda g: pl.semaphore_signal(barrier, inc=1, device_id=(g, p), device_id_type=MESH))

    def hop(d, h, sub):
        src, dst = (h - 1, h) if d == 0 else ((9 - h) % 8, 8 - h)
        part = pl.ds(sub * rows, rows)
        return pltpu.make_async_remote_copy(
            src_ref=held[src].at[part], dst_ref=held[dst].at[part],
            send_sem=zsend.at[d, h - 1, sub], recv_sem=zrecv.at[d, h - 1, sub],
            device_id=(me, left if d == 0 else right), device_id_type=MESH)

    def used(d, h, sub):
        return h < 4 or (h == 4 and (sub < SUBS // 2) == (d == 0))

    def pick(k):
        block = held[k]

        def some(t, c):
            for i in range(batch):
                g = t * batch + i
                for s in range(4):
                    send[k, g, s] = block[lists[p, s, g]]
            return c

        lax.fori_loop(0, G // batch, some, 0)

    def push(k):
        def one(g):
            pltpu.make_async_remote_copy(
                src_ref=send.at[k, g], dst_ref=land.at[k, me], send_sem=ssem.at[k], recv_sem=rsem.at[k],
                device_id=(g, p), device_id_type=MESH).start()

        pltpu.make_async_copy(send.at[k, me], land.at[k, me], rsem.at[k]).start()
        each_peer(one)

    for jj in range(2):
        for half in range(2):
            for xx in range(2):
                r = 4 * jj + 2 * half + xx
                lane = jj * 256 + half * 128
                wide[r * pitch:r * pitch + norb, :] = orb[xx, :, lane:lane + 128].astype(f32)

    def regroup(t, c):
        for i in range(8):
            o = t * 8 + i
            held[0][o] = wide[pl.ds(o, 8, stride=pitch), :].astype(bf16)
        return c

    lax.fori_loop(0, norb // 8, regroup, 0)
    pick(0)
    pl.semaphore_wait(barrier, G + 1)
    for sub in range(SUBS):
        for d in range(2):
            hop(d, 1, sub).start()
    push(0)
    for h in range(1, 5):
        for sub in range(SUBS):
            for d in range(2):
                if used(d, h, sub):
                    hop(d, h, sub).wait_recv()
                    if used(d, h + 1, sub):
                        hop(d, h + 1, sub).start()
        for k in (h, 8 - h) if h < 4 else (h,):
            pick(k)
            push(k)

    for k in (0, 1, 7, 2, 6, 3, 5, 4):
        pltpu.make_async_copy(land.at[k], land.at[k], rsem.at[k]).wait()

        def widen(t, c):
            for i in range(batch):
                g = t * batch + i
                for s in range(4):
                    F[pl.ds(pl.multiple_of(g * PITCH3, 4) + 8 * s, 8), :] = land[k, g, s].astype(f32)
            return c

        lax.fori_loop(0, G // batch, widen, 0)
        j = (p + k) % 8 * 2
        for s in range(4):
            for jj in range(2):
                for half in range(2):
                    for xx in range(2):
                        part = F[pl.ds(8 * s + 4 * jj + 2 * half + xx, G, stride=PITCH3), :]
                        box[s, j + jj, xx * G:(xx + 1) * G, half * 128:(half + 1) * 128] = part.astype(bf16)
    for h in range(1, 5):
        for sub in range(SUBS):
            for d in range(2):
                if used(d, h, sub):
                    hop(d, h, sub).wait_send()
    for k in range(8):
        pltpu.make_async_remote_copy(
            src_ref=send.at[k, pl.ds(1, G - 1)], dst_ref=land.at[k, pl.ds(1, G - 1)],
            send_sem=ssem.at[k], recv_sem=rsem.at[k], device_id=(me, right), device_id_type=MESH).wait_send()


def gather_boxes(orb, lists, gy, gx):
    G = gy * gx * 2
    norb = orb.shape[1]
    vmem = pl.BlockSpec(memory_space=pltpu.VMEM)
    return pl.pallas_call(
        lambda *refs: gather_kernel(gy, gx, *refs),
        out_shape=jax.ShapeDtypeStruct((4, 16, 2 * G, 256), bf16),
        in_specs=[vmem, pl.BlockSpec(memory_space=pltpu.SMEM)],
        out_specs=vmem,
        scratch_shapes=[pltpu.VMEM((norb, 8, 128), bf16)] * 8 + [
            pltpu.VMEM((9 * (norb + 4), 128), f32),
            pltpu.VMEM(((G + 1) * PITCH3, 128), f32),
            pltpu.VMEM((8, G, 4, 8, 128), bf16),
            pltpu.VMEM((8, G, 4, 8, 128), bf16),
            pltpu.SemaphoreType.DMA((2, 4, SUBS)),
            pltpu.SemaphoreType.DMA((2, 4, SUBS)),
            pltpu.SemaphoreType.DMA((8,)),
            pltpu.SemaphoreType.DMA((8,)),
        ],
        compiler_params=pltpu.CompilerParams(collective_id=0, has_side_effects=True, vmem_limit_bytes=16 << 20),
        cost_estimate=pl.CostEstimate(flops=20_000_000_000, bytes_accessed=60_000_000, transcendentals=0),
        name="gather_boxes",
    )(orb, lists)


ORDER = ((4, None), (3, None), (5, None), (2, None), (6, None), (1, None), (7, None), (0, None))
NF, NS = 3, 5


def collect_kernel(gy, gx, norb, col, lists, out, F, fields, keys, rows, bufa, bufb, bufc, bufd, sumc, sumd, hot, hotc,
                   ssem, rsem, zsend, zrecv):
    G = gy * gx * 2
    HG = G // 2
    K = G * 16
    R = 4 * norb
    me = lax.axis_index("grid")
    p = lax.axis_index("pair")
    my_y, my_x, my_c = me // (2 * gx), (me // 2) % gx, me % 2
    toward = ((p + 1) % 8, (p + 7) % 8)

    across = [((my_x + i // 2) % gx) * 2 + (my_c + i) % 2 for i in range(2 * gx)]

    def each_peer(act):
        for i in range(1, 2 * gx):
            act(my_y * (2 * gx) + across[i])

        def line(i, c):
            y = (my_y + i) % gy * (2 * gx)
            for a in across:
                act(y + a)
            return c

        lax.fori_loop(1, gy, line, 0)

    barrier = pltpu.get_barrier_semaphore()
    for z in toward:
        pl.semaphore_signal(barrier, inc=1, device_id=(me, z), device_id_type=MESH)

    each_peer(lambda g: pl.semaphore_signal(barrier, inc=1, device_id=(g, p), device_id_type=MESH))

    def choose(q, lo, n):
        key = keys[pl.ds(q, 1), lo:lo + n]
        rowid = lax.broadcasted_iota(jnp.int32, (R, n), 0)
        return jnp.where(rowid == key, jnp.float32(1), jnp.float32(0)).astype(bf16)

    batch = min(4, G)

    def deliver(k):
        j = (p + k) % 8 * 2
        for s in range(4):
            for jj in range(2):
                for half in range(2):
                    for xx in range(2):
                        F[pl.ds(G * PITCH2 * half + 4 * s + 2 * jj + xx, G, stride=PITCH2), :] = (
                            col[s, j + jj, xx * G:(xx + 1) * G, half * 128:(half + 1) * 128])

        def narrow(t, c):
            for i in range(batch):
                g = t * batch + i
                for half in range(2):
                    fields[k, g, half] = F[pl.ds(pl.multiple_of((half * G + g) * PITCH2, 4), 16), :].astype(bf16)
            return c

        lax.fori_loop(0, G // batch, narrow, 0)

    deliver(ORDER[0][0])
    pl.semaphore_wait(barrier, G + 1)

    def view(ref, k, g, h):
        return ref.at[k, g] if h is None else ref.at[k, g, h]

    def slot(k, h):
        return k

    def spread(k, h=None):
        sem = slot(k, h)
        pltpu.make_async_copy(view(fields, k, me, h), view(rows, k, me, h), rsem.at[sem]).start()

        def push(g):
            pltpu.make_async_remote_copy(
                src_ref=view(fields, k, g, h), dst_ref=view(rows, k, me, h), send_sem=ssem.at[sem],
                recv_sem=rsem.at[sem], device_id=(g, p), device_id_type=MESH).start()

        each_peer(push)

    def landed(k, h=None):
        part = view(rows, k, slice(None), h)
        pltpu.make_async_copy(part, part, rsem.at[slot(k, h)]).wait()

    def hop(d, stage, h):
        if stage == 0:
            src, dst = rows.at[4, pl.ds(d * HG, HG), h], bufa.at[d, h]
        elif stage == 1:
            src, dst = rows.at[(3, 5)[d], :, h], bufb.at[d, h, pl.ds(0, G)]
        elif stage == 2:
            src, dst = bufa.at[d, h], bufb.at[d, h, pl.ds(G, HG)]
        elif stage == 3:
            src, dst = sumc.at[d, h], bufc.at[d, h]
        else:
            src, dst = sumd.at[d, h], bufd.at[d, h]
        return pltpu.make_async_remote_copy(
            src_ref=src, dst_ref=dst, send_sem=zsend.at[d, stage, h], recv_sem=zrecv.at[d, stage, h],
            device_id=(me, toward[d]), device_id_type=MESH)

    def own(k, h):
        return mm(hot[...], rows[k, :, h].reshape(K, 128))

    def spread_many(lo, hi):
        for n in range(lo, hi):
            if n + 1 < len(ORDER):
                deliver(ORDER[n + 1][0])
            spread(*ORDER[n])

    spread_many(0, NF)
    col_g = lax.broadcasted_iota(jnp.int32, (G, K), 1)
    row_g = lax.broadcasted_iota(jnp.int32, (G, K), 0)
    all_keys = ((lax.broadcasted_iota(jnp.int32, (8, K), 1) % 4) * norb).astype(f32)
    for s in range(4):
        pattern = (col_g // 16 == row_g) & (col_g // 4 % 4 == s)
        pattern = jnp.where(pattern, jnp.float32(1), jnp.float32(0)).astype(bf16)
        all_keys = all_keys + mm(lists[:, s, :].astype(f32).astype(bf16), pattern)
    keys[...] = all_keys.astype(jnp.int32)

    hot[...] = choose(p, 0, K)
    landed(4)
    for h in range(2):
        for d in range(2):
            hop(d, 0, h).start()
    spread_many(NF, NS)
    for d in range(2):
        q1, q2 = ((p + 7) % 8, (p + 6) % 8) if d == 0 else ((p + 1) % 8, (p + 2) % 8)
        hotc[d, :, 0:K] = choose(q1, 0, K)
        hotc[d, :, K:K + K // 2] = choose(q2, d * (K // 2), K // 2)
    for h in range(2):
        for d in range(2):
            if h == 0:
                landed((3, 5)[d])
            hop(d, 1, h).start()
            hop(d, 0, h).wait_recv()
            hop(d, 2, h).start()
    spread_many(NS, len(ORDER))
    landed(2)
    landed(6)
    for h in range(2):
        for d in range(2):
            hop(d, 1, h).wait_recv()
            hop(d, 2, h).wait_recv()
            sumc[d, h] = own((2, 6)[d], h) + mm(hotc[d], bufb[d, h].reshape(K + K // 2, 128))
            hop(d, 3, h).start()
    landed(1)
    landed(7)
    landed(0)
    mine = [own(0, h) for h in range(2)]
    for h in range(2):
        for d in range(2):
            part = own((1, 7)[d], h)
            hop(d, 3, h).wait_recv()
            sumd[d, h] = (part + bufc[d, h]).astype(bf16)
            hop(d, 4, h).start()
    for h in range(2):
        for d in range(2):
            hop(d, 4, h).wait_recv()
        total = mine[h] + bufd[0, h].astype(f32) + bufd[1, h].astype(f32)
        for jj in range(2):
            for xx in range(2):
                i = jj * 2 + xx
                out[xx, :, jj * 256 + h * 128:jj * 256 + (h + 1) * 128] = total[i * norb:(i + 1) * norb]
    for d in range(2):
        for stage in range(5):
            for h in range(2):
                hop(d, stage, h).wait_send()
    for k, h in ORDER:
        many = pl.ds(1, G - 1)
        pltpu.make_async_remote_copy(
            src_ref=view(fields, k, many, h), dst_ref=view(rows, k, many, h), send_sem=ssem.at[slot(k, h)],
            recv_sem=rsem.at[slot(k, h)], device_id=(me, toward[0]), device_id_type=MESH).wait_send()


def collect_fields(col, lists, norb, gy, gx):
    G = gy * gx * 2
    vmem = pl.BlockSpec(memory_space=pltpu.VMEM)
    sums = pltpu.VMEM((2, 2, 4 * norb, 128), f32)
    last = pltpu.VMEM((2, 2, 4 * norb, 128), bf16)
    return pl.pallas_call(
        lambda *refs: collect_kernel(gy, gx, norb, *refs),
        out_shape=jax.ShapeDtypeStruct((2, norb, 512), f32),
        in_specs=[vmem, vmem],
        out_specs=vmem,
        scratch_shapes=[
            pltpu.VMEM(((2 * G + 1) * PITCH2, 128), f32),
            pltpu.VMEM((8, G, 2, 16, 128), bf16),
            pltpu.VMEM((8, G * 16), jnp.int32),
            pltpu.VMEM((8, G, 2, 16, 128), bf16),
            pltpu.VMEM((2, 2, G // 2, 16, 128), bf16),
            pltpu.VMEM((2, 2, G + G // 2, 16, 128), bf16),
            sums, last, sums, last,
            pltpu.VMEM((4 * norb, G * 16), bf16),
            pltpu.VMEM((2, 4 * norb, G * 24), bf16),
            pltpu.SemaphoreType.DMA((10,)),
            pltpu.SemaphoreType.DMA((10,)),
            pltpu.SemaphoreType.DMA((2, 5, 2)),
            pltpu.SemaphoreType.DMA((2, 5, 2)),
        ],
        compiler_params=pltpu.CompilerParams(collective_id=1, has_side_effects=True, vmem_limit_bytes=22 << 20),
        name="collect_fields",
    )(col, lists)


def shards(orbitals, box_list, pair_slots, offsets, pair_count):
    lists = jnp.transpose(box_list, (1, 2, 0))
    slots = jnp.transpose(pair_slots, (0, 1, 3, 2)).reshape(2, 4)
    offs = jnp.transpose(offsets, (0, 3, 1, 2)).reshape(3, 1, 4)
    box = gather_boxes(orbitals, lists, 4, 4)
    col = worker_fields(box, slots, offs, pair_count)
    return collect_fields(col, lists, orbitals.shape[1], 4, 4)


def solution(mesh):
    placed = (
        P("grid", None, "pair"),
        P(),
        P("grid", "pair", None, None),
        P("grid", "pair", None, None),
        P("grid", "pair"),
    )
    return jax.shard_map(
        shards, mesh=mesh, in_specs=placed, out_specs=P("grid", None, "pair"), check_vma=False
    )
```

```python
import math
import numpy as np
import jax
import jax.numpy as jnp
from jax import lax
from jax.experimental import pallas as pl
from jax.experimental.pallas import tpu as pltpu
from jax.sharding import PartitionSpec as P

screening = 0.02
N = 64
CH = 16
W = 256
PITCH = 68
PITCH2 = 20
PITCH3 = 36
f32, bf16 = jnp.float32, jnp.bfloat16


def tables():
    m = np.arange(N)
    ph = 2.0 * math.pi * ((m[:, None] * m[None, :]) % N) / N
    cas = np.cos(ph) + np.sin(ph)
    perm = np.concatenate([np.arange(0, N, 2), np.arange(1, N, 2)])

    def parts(a):
        a = np.asarray(a, np.float32)
        hi = a.astype(bf16)
        lo = (a - hi.astype(np.float32)).astype(bf16)
        return hi, lo

    def left(a):
        hi, lo = parts(a)
        return np.concatenate([hi, hi, lo], axis=1)

    cx = left(cas[:, perm])
    ux = left(cas[perm, :])
    cf = left(cas[:, perm])
    ci = left(cas[perm, :])
    hi, lo = parts(np.kron(np.eye(4), cas))
    bd = np.concatenate([hi, hi, lo], axis=0)
    e = 2.0 - 2.0 * np.cos(2.0 * math.pi * m / N)
    green = 1.0 / ((screening + e[:, None, None] + e[None, :, None] + e[None, None, :]) * float(N**3))
    g = green.reshape(CH, 4, N, N).transpose(0, 2, 1, 3).reshape(CH, N, W).astype(np.float32)
    return cx, ux, bd, g


def split(v):
    hi = v.astype(bf16)
    lo = (v - hi.astype(f32)).astype(bf16)
    return hi, lo


def mm(a, b):
    return jnp.dot(a, b, preferred_element_type=f32)


def left_mul(table, v):
    hi, lo = split(v)
    return mm(table, jnp.concatenate([hi, lo, hi], axis=0))


def right_mul(v, bd):
    hi, lo = split(v)
    return mm(jnp.concatenate([hi, lo, hi], axis=1), bd)


def pair_kernel(slots, offs, count, box, cx, ux, bd, green, col, S, SH, U):
    low = lax.broadcasted_iota(jnp.int32, (32, 128), 1) < 64
    lane = lax.broadcasted_iota(jnp.int32, (N, 128), 1)
    for r in (slice(0, 6), slice(38, 44)):
        S[r] = jnp.zeros((6, 96, 128), f32)
    for r in (0, 40, 48, 88):
        S[6:38, r:r + 8, :] = jnp.zeros((32, 8, 128), f32)
    col[...] = jnp.zeros(col.shape, f32)

    def pair(k, carry):
        a = slots[0, k]
        b = slots[1, k]
        dx, dy, dz = offs[0, 0, k], offs[1, 0, k], offs[2, 0, k]
        t = dy * 64 + dz
        q = (t + 1024) // 128 - 8
        r = t - 128 * q
        z = lane % 64
        inside = (z + dz >= 0) & (z + dz < 64)
        inside_back = (z - dz >= 0) & (z - dz < 64)

        def put(j, v):
            for h in range(2):
                for e in range(2):
                    S[6 + 2 * j + h, e * 48 + 8:e * 48 + 40, :] = v[e * 32:(e + 1) * 32, h * 128:(h + 1) * 128]

        def fetch(tile, step, turn):
            both = []
            for e in range(2):
                n = step + 16 + e
                both.append(S[tile, pl.ds(n % 2 * 48 + n // 2, 32), :])
            return pltpu.roll(jnp.concatenate(both, axis=0), turn, 1)

        for j in range(CH):
            put(j, box[b, j].astype(f32))
        turn = (128 - r) % 128
        here = fetch(6 + q, dx, turn)
        for T in range(2 * CH):
            then = fetch(7 + T + q, dx, turn)
            SH[T] = jnp.where(inside, jnp.where(lane < 128 - r, here, then), jnp.float32(0))
            here = then

        outs = []
        for j in range(CH):
            moved = jnp.concatenate([SH[2 * j], SH[2 * j + 1]], axis=1)
            outs.append(left_mul(cx[...], box[a, j].astype(f32) * moved))
        spec = right_mul(jnp.concatenate(outs, axis=0), bd[...])
        for j in range(CH):
            for h in range(2):
                U[(2 * j + h) * PITCH:(2 * j + h) * PITCH + N, :] = spec[j * N:(j + 1) * N, h * 128:(h + 1) * 128]

        def middle(g, c):
            tops, bots = [], []
            for h in range(2):
                l1 = U[pl.ds(g * 4 + 2 * h, 32, stride=PITCH), :]
                l2 = U[pl.ds(g * 4 + 2 * h + 1, 32, stride=PITCH), :]
                tops.append(jnp.where(low, l1, pltpu.roll(l2, 64, 1)))
                bots.append(jnp.where(low, pltpu.roll(l1, 64, 1), l2))
            v = jnp.concatenate([jnp.concatenate(tops, axis=1), jnp.concatenate(bots, axis=1)], axis=0)
            s = left_mul(cx[...], v) * green[g]
            p = left_mul(ux[...], s)
            for h in range(2):
                x0 = p[:32, h * 128:(h + 1) * 128]
                x1 = p[32:, h * 128:(h + 1) * 128]
                U[pl.ds(g * 4 + 2 * h, 32, stride=PITCH), :] = jnp.where(low, x0, pltpu.roll(x1, 64, 1))
                U[pl.ds(g * 4 + 2 * h + 1, 32, stride=PITCH), :] = jnp.where(low, pltpu.roll(x0, 64, 1), x1)
            return c

        lax.fori_loop(0, CH, middle, 0, unroll=8)

        outs = []
        for j in range(CH):
            v = jnp.concatenate([U[(2 * j + h) * PITCH:(2 * j + h) * PITCH + N, :] for h in range(2)], axis=1)
            outs.append(left_mul(ux[...], v))
        pot = right_mul(jnp.concatenate(outs, axis=0), bd[...]).reshape(CH, N, W)
        for j in range(CH):
            moved = jnp.concatenate([SH[2 * j], SH[2 * j + 1]], axis=1)
            col[a, j] = col[a, j] - pot[j] * moved
            put(j, -(pot[j] * box[a, j].astype(f32)))

        here = fetch(5 - q, -dx, r)
        for T in range(2 * CH):
            then = fetch(6 + T - q, -dx, r)
            u = jnp.where(inside_back, jnp.where(lane < r, here, then), jnp.float32(0))
            part = slice(T % 2 * 128, T % 2 * 128 + 128)
            col[b, T // 2, :, part] = col[b, T // 2, :, part] + u
            here = then
        return carry

    lax.fori_loop(0, count[0, 0], pair, 0)


def worker_fields(box, slots, offs, count):
    cx, ux, bd, g = (jnp.asarray(t) for t in tables())
    smem = pl.BlockSpec(memory_space=pltpu.SMEM)
    vmem = pl.BlockSpec(memory_space=pltpu.VMEM)
    return pl.pallas_call(
        pair_kernel,
        out_shape=jax.ShapeDtypeStruct((4, CH, N, W), f32),
        in_specs=[smem] * 3 + [vmem] * 5,
        out_specs=vmem,
        scratch_shapes=[
            pltpu.VMEM((44, 96, 128), f32),
            pltpu.VMEM((2 * CH, N, 128), f32),
            pltpu.VMEM((33 * PITCH, 128), f32),
        ],
        compiler_params=pltpu.CompilerParams(vmem_limit_bytes=28 << 20),
        name="pairs",
    )(slots, offs, count, box, cx, ux, bd, g)


MESH = pl.DeviceIdType.MESH
SUBS = 2


def gather_kernel(gy, gx, orb, lists, box, *rest):
    blocks = rest[:8]
    wide, F, land, send, zsend, zrecv, ssem, rsem = rest[8:]
    G = gy * gx * 2
    me = lax.axis_index("grid")
    p = lax.axis_index("pair")
    my_y, my_x, my_c = me // (2 * gx), (me // 2) % gx, me % 2
    right, left = (p + 1) % 8, (p + 7) % 8
    held = blocks
    norb = orb.shape[1]
    pitch = norb + 4
    rows = norb // SUBS
    batch = min(4, G)

    across = [((my_x + i // 2) % gx) * 2 + (my_c + i) % 2 for i in range(2 * gx)]

    def each_peer(act):
        for i in range(1, 2 * gx):
            act(my_y * (2 * gx) + across[i])

        def line(i, c):
            y = (my_y + i) % gy * (2 * gx)
            for a in across:
                act(y + a)
            return c

        lax.fori_loop(1, gy, line, 0)

    barrier = pltpu.get_barrier_semaphore()
    pl.semaphore_signal(barrier, inc=1, device_id=(me, right), device_id_type=MESH)
    pl.semaphore_signal(barrier, inc=1, device_id=(me, left), device_id_type=MESH)

    each_peer(lambda g: pl.semaphore_signal(barrier, inc=1, device_id=(g, p), device_id_type=MESH))

    def hop(d, h, sub):
        src, dst = (h - 1, h) if d == 0 else ((9 - h) % 8, 8 - h)
        part = pl.ds(sub * rows, rows)
        return pltpu.make_async_remote_copy(
            src_ref=held[src].at[part], dst_ref=held[dst].at[part],
            send_sem=zsend.at[d, h - 1, sub], recv_sem=zrecv.at[d, h - 1, sub],
            device_id=(me, left if d == 0 else right), device_id_type=MESH)

    def used(d, h, sub):
        return h < 4 or (h == 4 and (sub < SUBS // 2) == (d == 0))

    def pick(k):
        block = held[k]

        def some(t, c):
            for i in range(batch):
                g = t * batch + i
                for s in range(4):
                    send[k, g, s] = block[lists[p, s, g]]
            return c

        lax.fori_loop(0, G // batch, some, 0)

    def push(k):
        def one(g):
            pltpu.make_async_remote_copy(
                src_ref=send.at[k, g], dst_ref=land.at[k, me], send_sem=ssem.at[k], recv_sem=rsem.at[k],
                device_id=(g, p), device_id_type=MESH).start()

        pltpu.make_async_copy(send.at[k, me], land.at[k, me], rsem.at[k]).start()
        each_peer(one)

    for jj in range(2):
        for half in range(2):
            for xx in range(2):
                r = 4 * jj + 2 * half + xx
                lane = jj * 256 + half * 128
                wide[r * pitch:r * pitch + norb, :] = orb[xx, :, lane:lane + 128].astype(f32)

    def regroup(t, c):
        for i in range(8):
            o = t * 8 + i
            held[0][o] = wide[pl.ds(o, 8, stride=pitch), :].astype(bf16)
        return c

    lax.fori_loop(0, norb // 8, regroup, 0)
    pick(0)
    pl.semaphore_wait(barrier, G + 1)
    for sub in range(SUBS):
        for d in range(2):
            hop(d, 1, sub).start()
    push(0)
    for h in range(1, 5):
        for sub in range(SUBS):
            for d in range(2):
                if used(d, h, sub):
                    hop(d, h, sub).wait_recv()
                    if used(d, h + 1, sub):
                        hop(d, h + 1, sub).start()
        for k in (h, 8 - h) if h < 4 else (h,):
            pick(k)
            push(k)

    for k in (0, 1, 7, 2, 6, 3, 5, 4):
        pltpu.make_async_copy(land.at[k], land.at[k], rsem.at[k]).wait()

        def widen(t, c):
            for i in range(batch):
                g = t * batch + i
                for s in range(4):
                    F[pl.ds(pl.multiple_of(g * PITCH3, 4) + 8 * s, 8), :] = land[k, g, s].astype(f32)
            return c

        lax.fori_loop(0, G // batch, widen, 0)
        j = (p + k) % 8 * 2
        for s in range(4):
            for jj in range(2):
                for half in range(2):
                    for xx in range(2):
                        part = F[pl.ds(8 * s + 4 * jj + 2 * half + xx, G, stride=PITCH3), :]
                        box[s, j + jj, xx * G:(xx + 1) * G, half * 128:(half + 1) * 128] = part.astype(bf16)
    for h in range(1, 5):
        for sub in range(SUBS):
            for d in range(2):
                if used(d, h, sub):
                    hop(d, h, sub).wait_send()
    for k in range(8):
        pltpu.make_async_remote_copy(
            src_ref=send.at[k, pl.ds(1, G - 1)], dst_ref=land.at[k, pl.ds(1, G - 1)],
            send_sem=ssem.at[k], recv_sem=rsem.at[k], device_id=(me, right), device_id_type=MESH).wait_send()


def gather_boxes(orb, lists, gy, gx):
    G = gy * gx * 2
    norb = orb.shape[1]
    vmem = pl.BlockSpec(memory_space=pltpu.VMEM)
    return pl.pallas_call(
        lambda *refs: gather_kernel(gy, gx, *refs),
        out_shape=jax.ShapeDtypeStruct((4, 16, 2 * G, 256), bf16),
        in_specs=[vmem, pl.BlockSpec(memory_space=pltpu.SMEM)],
        out_specs=vmem,
        scratch_shapes=[pltpu.VMEM((norb, 8, 128), bf16)] * 8 + [
            pltpu.VMEM((9 * (norb + 4), 128), f32),
            pltpu.VMEM(((G + 1) * PITCH3, 128), f32),
            pltpu.VMEM((8, G, 4, 8, 128), bf16),
            pltpu.VMEM((8, G, 4, 8, 128), bf16),
            pltpu.SemaphoreType.DMA((2, 4, SUBS)),
            pltpu.SemaphoreType.DMA((2, 4, SUBS)),
            pltpu.SemaphoreType.DMA((8,)),
            pltpu.SemaphoreType.DMA((8,)),
        ],
        compiler_params=pltpu.CompilerParams(collective_id=0, has_side_effects=True, vmem_limit_bytes=16 << 20),
        cost_estimate=pl.CostEstimate(flops=20_000_000_000, bytes_accessed=60_000_000, transcendentals=0),
        name="gather_boxes",
    )(orb, lists)


ORDER = ((4, None), (3, None), (5, None), (2, None), (6, None), (1, None), (7, None), (0, None))
NF, NS = 3, 5


def collect_kernel(gy, gx, norb, col, lists, out, F, fields, keys, rows, bufa, bufb, bufc, bufd, sumc, sumd, hot, hotc,
                   ssem, rsem, zsend, zrecv):
    G = gy * gx * 2
    HG = G // 2
    K = G * 16
    R = 4 * norb
    me = lax.axis_index("grid")
    p = lax.axis_index("pair")
    my_y, my_x, my_c = me // (2 * gx), (me // 2) % gx, me % 2
    toward = ((p + 1) % 8, (p + 7) % 8)

    across = [((my_x + i // 2) % gx) * 2 + (my_c + i) % 2 for i in range(2 * gx)]

    def each_peer(act):
        for i in range(1, 2 * gx):
            act(my_y * (2 * gx) + across[i])

        def line(i, c):
            y = (my_y + i) % gy * (2 * gx)
            for a in across:
                act(y + a)
            return c

        lax.fori_loop(1, gy, line, 0)

    barrier = pltpu.get_barrier_semaphore()
    for z in toward:
        pl.semaphore_signal(barrier, inc=1, device_id=(me, z), device_id_type=MESH)

    each_peer(lambda g: pl.semaphore_signal(barrier, inc=1, device_id=(g, p), device_id_type=MESH))

    def choose(q, lo, n):
        key = keys[pl.ds(q, 1), lo:lo + n]
        rowid = lax.broadcasted_iota(jnp.int32, (R, n), 0)
        return jnp.where(rowid == key, jnp.float32(1), jnp.float32(0)).astype(bf16)

    batch = min(4, G)

    def deliver(k):
        j = (p + k) % 8 * 2
        for s in range(4):
            for jj in range(2):
                for half in range(2):
                    for xx in range(2):
                        F[pl.ds(G * PITCH2 * half + 4 * s + 2 * jj + xx, G, stride=PITCH2), :] = (
                            col[s, j + jj, xx * G:(xx + 1) * G, half * 128:(half + 1) * 128])

        def narrow(t, c):
            for i in range(batch):
                g = t * batch + i
                for half in range(2):
                    fields[k, g, half] = F[pl.ds(pl.multiple_of((half * G + g) * PITCH2, 4), 16), :].astype(bf16)
            return c

        lax.fori_loop(0, G // batch, narrow, 0)

    deliver(ORDER[0][0])
    pl.semaphore_wait(barrier, G + 1)

    def view(ref, k, g, h):
        return ref.at[k, g] if h is None else ref.at[k, g, h]

    def slot(k, h):
        return k

    def spread(k, h=None):
        sem = slot(k, h)
        pltpu.make_async_copy(view(fields, k, me, h), view(rows, k, me, h), rsem.at[sem]).start()

        def push(g):
            pltpu.make_async_remote_copy(
                src_ref=view(fields, k, g, h), dst_ref=view(rows, k, me, h), send_sem=ssem.at[sem],
                recv_sem=rsem.at[sem], device_id=(g, p), device_id_type=MESH).start()

        each_peer(push)

    def landed(k, h=None):
        part = view(rows, k, slice(None), h)
        pltpu.make_async_copy(part, part, rsem.at[slot(k, h)]).wait()

    def hop(d, stage, h):
        if stage == 0:
            src, dst = rows.at[4, pl.ds(d * HG, HG), h], bufa.at[d, h]
        elif stage == 1:
            src, dst = rows.at[(3, 5)[d], :, h], bufb.at[d, h, pl.ds(0, G)]
        elif stage == 2:
            src, dst = bufa.at[d, h], bufb.at[d, h, pl.ds(G, HG)]
        elif stage == 3:
            src, dst = sumc.at[d, h], bufc.at[d, h]
        else:
            src, dst = sumd.at[d, h], bufd.at[d, h]
        return pltpu.make_async_remote_copy(
            src_ref=src, dst_ref=dst, send_sem=zsend.at[d, stage, h], recv_sem=zrecv.at[d, stage, h],
            device_id=(me, toward[d]), device_id_type=MESH)

    def own(k, h):
        return mm(hot[...], rows[k, :, h].reshape(K, 128))

    def spread_many(lo, hi):
        for n in range(lo, hi):
            if n + 1 < len(ORDER):
                deliver(ORDER[n + 1][0])
            spread(*ORDER[n])

    spread_many(0, NF)
    col_g = lax.broadcasted_iota(jnp.int32, (G, K), 1)
    row_g = lax.broadcasted_iota(jnp.int32, (G, K), 0)
    all_keys = ((lax.broadcasted_iota(jnp.int32, (8, K), 1) % 4) * norb).astype(f32)
    for s in range(4):
        pattern = (col_g // 16 == row_g) & (col_g // 4 % 4 == s)
        pattern = jnp.where(pattern, jnp.float32(1), jnp.float32(0)).astype(bf16)
        all_keys = all_keys + mm(lists[:, s, :].astype(f32).astype(bf16), pattern)
    keys[...] = all_keys.astype(jnp.int32)

    hot[...] = choose(p, 0, K)
    landed(4)
    for h in range(2):
        for d in range(2):
            hop(d, 0, h).start()
    spread_many(NF, NS)
    for d in range(2):
        q1, q2 = ((p + 7) % 8, (p + 6) % 8) if d == 0 else ((p + 1) % 8, (p + 2) % 8)
        hotc[d, :, 0:K] = choose(q1, 0, K)
        hotc[d, :, K:K + K // 2] = choose(q2, d * (K // 2), K // 2)
    for h in range(2):
        for d in range(2):
            if h == 0:
                landed((3, 5)[d])
            hop(d, 1, h).start()
            hop(d, 0, h).wait_recv()
            hop(d, 2, h).start()
    spread_many(NS, len(ORDER))
    landed(2)
    landed(6)
    for h in range(2):
        for d in range(2):
            hop(d, 1, h).wait_recv()
            hop(d, 2, h).wait_recv()
            sumc[d, h] = own((2, 6)[d], h) + mm(hotc[d], bufb[d, h].reshape(K + K // 2, 128))
            hop(d, 3, h).start()
    landed(1)
    landed(7)
    landed(0)
    mine = [own(0, h) for h in range(2)]
    for h in range(2):
        for d in range(2):
            part = own((1, 7)[d], h)
            hop(d, 3, h).wait_recv()
            sumd[d, h] = (part + bufc[d, h]).astype(bf16)
            hop(d, 4, h).start()
    for h in range(2):
        for d in range(2):
            hop(d, 4, h).wait_recv()
        total = mine[h] + bufd[0, h].astype(f32) + bufd[1, h].astype(f32)
        for jj in range(2):
            for xx in range(2):
                i = jj * 2 + xx
                out[xx, :, jj * 256 + h * 128:jj * 256 + (h + 1) * 128] = total[i * norb:(i + 1) * norb]
    for d in range(2):
        for stage in range(5):
            for h in range(2):
                hop(d, stage, h).wait_send()
    for k, h in ORDER:
        many = pl.ds(1, G - 1)
        pltpu.make_async_remote_copy(
            src_ref=view(fields, k, many, h), dst_ref=view(rows, k, many, h), send_sem=ssem.at[slot(k, h)],
            recv_sem=rsem.at[slot(k, h)], device_id=(me, toward[0]), device_id_type=MESH).wait_send()


def collect_fields(col, lists, norb, gy, gx):
    G = gy * gx * 2
    vmem = pl.BlockSpec(memory_space=pltpu.VMEM)
    sums = pltpu.VMEM((2, 2, 4 * norb, 128), f32)
    last = pltpu.VMEM((2, 2, 4 * norb, 128), bf16)
    return pl.pallas_call(
        lambda *refs: collect_kernel(gy, gx, norb, *refs),
        out_shape=jax.ShapeDtypeStruct((2, norb, 512), f32),
        in_specs=[vmem, vmem],
        out_specs=vmem,
        scratch_shapes=[
            pltpu.VMEM(((2 * G + 1) * PITCH2, 128), f32),
            pltpu.VMEM((8, G, 2, 16, 128), bf16),
            pltpu.VMEM((8, G * 16), jnp.int32),
            pltpu.VMEM((8, G, 2, 16, 128), bf16),
            pltpu.VMEM((2, 2, G // 2, 16, 128), bf16),
            pltpu.VMEM((2, 2, G + G // 2, 16, 128), bf16),
            sums, last, sums, last,
            pltpu.VMEM((4 * norb, G * 16), bf16),
            pltpu.VMEM((2, 4 * norb, G * 24), bf16),
            pltpu.SemaphoreType.DMA((10,)),
            pltpu.SemaphoreType.DMA((10,)),
            pltpu.SemaphoreType.DMA((2, 5, 2)),
            pltpu.SemaphoreType.DMA((2, 5, 2)),
        ],
        compiler_params=pltpu.CompilerParams(collective_id=1, has_side_effects=True, vmem_limit_bytes=22 << 20),
        name="collect_fields",
    )(col, lists)


def shards(orbitals, box_list, pair_slots, offsets, pair_count):
    lists = jnp.transpose(box_list, (1, 2, 0))
    slots = jnp.transpose(pair_slots, (0, 1, 3, 2)).reshape(2, 4)
    offs = jnp.transpose(offsets, (0, 3, 1, 2)).reshape(3, 1, 4)
    box = gather_boxes(orbitals, lists, 4, 4)
    col = worker_fields(box, slots, offs, pair_count)
    return collect_fields(col, lists, orbitals.shape[1], 4, 4)


def solution(mesh):
    placed = (
        P("grid", None, "pair"),
        P(),
        P("grid", "pair", None, None),
        P("grid", "pair", None, None),
        P("grid", "pair"),
    )
    return jax.shard_map(
        shards, mesh=mesh, in_specs=placed, out_specs=P("grid", None, "pair"), check_vma=False
    )
```
